16 devices in a mesh: rep: 4 (over z, y), shard: 4 (over x, core).
Axes of the slice: x: 2, y: 2, z: 2, core: 2. Of those that a mesh axis runs over, the one named last changes fastest.
Arguments:
- ratings: float32 [10240, 512], P(('rep', 'shard')), parts along dimension 0
- obs_mask: int32 [10240, 512], P(('rep', 'shard')), parts along dimension 0
- step_counts: int32 [16, 4], P(('rep', 'shard')), parts along dimension 0
- user_init: float32 [10240, 256], P(('rep', 'shard')), parts along dimension 0
- item_init: float32 [2048, 256], P(('rep', 'shard')), parts along dimension 0
Outputs:
- output 1: float32 [10240, 256], P(('rep', 'shard')), parts along dimension 0
- output 2: float32 [2048, 256], P(('rep', 'shard')), parts along dimension 0
There are 4 independent parts. The reference program is written for one: setup_inputs(seed, part) draws one part's arguments, and reference() takes and returns one part's arrays. A program takes and returns all parts, laid end to end along the dimension named above; each array names one.
All inputs are finite; a program needn't handle non-finite values.
Results may differ from the reference program's by a relative error of at most 0.00155027.
Values are sent between devices in bfloat16 or wider.
A program may use at most 1 GiB of HBM per device.

```python
import math
import jax
import jax.numpy as jnp
from jax import lax

GROUP_SIZE = 4
FACTOR_RANK = 256
ASPECT = 5
ITEMS_DEV = 128
STEPS_MAX = 4
EPOCHS = 2

USERS_DEV = ASPECT * ITEMS_DEV
NUM_USERS = GROUP_SIZE * USERS_DEV
NUM_ITEMS = GROUP_SIZE * ITEMS_DEV
TRUE_RANK = FACTOR_RANK // 4
STEP_SIZE = 0.4 * math.sqrt(FACTOR_RANK) / (USERS_DEV + FACTOR_RANK)
DECAY_RATE = 0.1 * ITEMS_DEV / math.sqrt(FACTOR_RANK)


def draw_layout(layout_key):
    key_list = jax.random.split(layout_key, 5)
    density_pct = jax.random.randint(key_list[0], (GROUP_SIZE, 1, GROUP_SIZE, 1), 10, 41)
    coin_draws = jax.random.randint(key_list[1], (GROUP_SIZE, USERS_DEV, GROUP_SIZE, ITEMS_DEV), 0, 100)
    obs_mask = (coin_draws < density_pct).astype(jnp.int32).reshape(NUM_USERS, NUM_ITEMS)
    slot_count = GROUP_SIZE * GROUP_SIZE
    step_flat = jax.random.randint(key_list[2], (slot_count,), 1, STEPS_MAX + 1)
    top_pos = jax.random.randint(key_list[3], (), 0, slot_count)
    low_pos = (top_pos + 1 + jax.random.randint(key_list[4], (), 0, slot_count - 1)) % slot_count
    slot_ids = jnp.arange(slot_count)
    step_flat = jnp.where(slot_ids == top_pos, STEPS_MAX, jnp.where(slot_ids == low_pos, 1, step_flat))
    return obs_mask, step_flat.reshape(GROUP_SIZE, GROUP_SIZE).astype(jnp.int32)


def setup_inputs(seed: int = 0, part: int = 0) -> dict:
    base_key = jax.random.fold_in(jax.random.key(seed), part)
    key_list = jax.random.split(base_key, 6)
    user_true = jax.random.normal(key_list[0], (NUM_USERS, TRUE_RANK), jnp.float32)
    item_true = jax.random.normal(key_list[1], (NUM_ITEMS, TRUE_RANK), jnp.float32)
    noise_term = 0.3 * jax.random.normal(key_list[2], (NUM_USERS, NUM_ITEMS), jnp.float32)
    ratings = jnp.dot(user_true, item_true.T) / math.sqrt(TRUE_RANK) + noise_term
    obs_mask, step_counts = draw_layout(key_list[3])
    factor_scale = FACTOR_RANK ** -0.25
    user_init = factor_scale * jax.random.normal(key_list[4], (NUM_USERS, FACTOR_RANK), jnp.float32)
    item_init = factor_scale * jax.random.normal(key_list[5], (NUM_ITEMS, FACTOR_RANK), jnp.float32)
    return {"ratings": ratings, "obs_mask": obs_mask, "step_counts": step_counts, "user_init": user_init, "item_init": item_init}


def reference(ratings, obs_mask, step_counts, user_init, item_init):
    rating_blocks = ratings.reshape(GROUP_SIZE, USERS_DEV, GROUP_SIZE, ITEMS_DEV)
    mask_blocks = obs_mask.reshape(GROUP_SIZE, USERS_DEV, GROUP_SIZE, ITEMS_DEV)
    user_blocks = user_init.reshape(GROUP_SIZE, USERS_DEV, FACTOR_RANK)
    item_blocks = item_init.reshape(GROUP_SIZE, ITEMS_DEV, FACTOR_RANK)
    row_ids = jnp.arange(GROUP_SIZE)

    def block_update(block_args):
        row_id, col_id, user_blk, item_blk = block_args
        rating_blk = rating_blocks[row_id, :, col_id, :]
        seen_blk = mask_blocks[row_id, :, col_id, :] != 0

        def grad_step(step_idx, inner_in):
            user_now, item_now = inner_in
            user_half = user_now.astype(jnp.bfloat16)
            item_half = item_now.astype(jnp.bfloat16)
            approx = jnp.dot(user_half, item_half.T, preferred_element_type=jnp.float32)
            err_half = jnp.where(seen_blk, approx - rating_blk, 0.0).astype(jnp.bfloat16)
            grad_user = jnp.dot(err_half, item_half, preferred_element_type=jnp.float32) + DECAY_RATE * user_now
            grad_item = jnp.dot(err_half.T, user_half, preferred_element_type=jnp.float32) + DECAY_RATE * item_now
            return user_now - STEP_SIZE * grad_user, item_now - STEP_SIZE * grad_item

        return lax.fori_loop(0, step_counts[row_id, col_id], grad_step, (user_blk, item_blk))

    def sub_epoch(sweep_idx, carry_in):
        user_cur, held_items = carry_in
        col_ids = (row_ids + sweep_idx) % GROUP_SIZE
        user_new, item_new = lax.map(block_update, (row_ids, col_ids, user_cur, held_items))
        return user_new, jnp.roll(item_new, -1, axis=0)

    user_fin, item_fin = lax.fori_loop(0, EPOCHS * GROUP_SIZE, sub_epoch, (user_blocks, item_blocks))
    return user_fin.reshape(NUM_USERS, FACTOR_RANK), item_fin.reshape(NUM_ITEMS, FACTOR_RANK)
```

```python
import math
import jax
import jax.numpy as jnp
from jax import lax
from jax.experimental import pallas as pl
from jax.experimental.pallas import tpu as pltpu
from jax.sharding import PartitionSpec as P

EPOCHS = 2
STEPS_MAX = 4
CHUNK = 128


def make_kernel(n, users, items, rank):
    step_size = 0.4 * math.sqrt(rank) / (users + rank)
    decay = 0.1 * items / math.sqrt(rank)
    keep = 1.0 - step_size * decay
    hops = EPOCHS * n
    bf16, f32 = jnp.bfloat16, jnp.float32
    starts = range(0, users, CHUNK)

    def kernel(cnt, r_hbm, m_hbm, u_hbm, v_hbm, u_out, v_out,
               r_buf, m_buf, u_f, u_b, v_slot, v_send, v_f, e_b,
               r_sem, m_sem, u_sem, recv_sem, send_sem, out_sem):
        me = lax.axis_index("shard")
        left, right = lax.rem(me + n - 1, n), lax.rem(me + 1, n)

        barrier = pltpu.get_barrier_semaphore()
        for peer in (left, right):
            pl.semaphore_signal(barrier, inc=1, device_id={"shard": peer}, device_id_type=pl.DeviceIdType.MESH)

        def block_copy(kind, q):
            src, dst, sem = ((r_hbm, r_buf, r_sem), (m_hbm, m_buf, m_sem))[kind]
            col = pl.multiple_of(lax.rem(me + q, n) * items, items)
            return pltpu.make_async_copy(src.at[:, pl.ds(col, items)], dst.at[q], sem.at[q])

        u_in = pltpu.make_async_copy(u_hbm, u_f, u_sem)
        v_in = pltpu.make_async_copy(v_hbm, v_slot.at[0], recv_sem.at[0])
        u_in.start()
        v_in.start()
        for q in range(n):
            block_copy(0, q).start()
            block_copy(1, q).start()
        u_in.wait()
        for s in starts:
            u_b[pl.ds(s, CHUNK), :] = u_f[pl.ds(s, CHUNK), :].astype(bf16)
        v_in.wait()
        pl.semaphore_wait(barrier, 2)

        def hop_copy(t):
            return pltpu.make_async_remote_copy(
                src_ref=v_send.at[t], dst_ref=v_slot.at[t + 1],
                send_sem=send_sem.at[t], recv_sem=recv_sem.at[t + 1],
                device_id={"shard": left}, device_id_type=pl.DeviceIdType.MESH)

        def sub_epoch(t, carry):
            q = lax.rem(t, n)
            count = cnt[0, lax.rem(me + t, n)]

            @pl.when(t < n)
            def _():
                block_copy(0, t).wait()
                block_copy(1, t).wait()

            @pl.when(t > 0)
            def _():
                pltpu.make_async_copy(v_slot.at[t], v_slot.at[t], recv_sem.at[t]).wait()

            for k in range(STEPS_MAX):
                v_old = (v_slot.at[t] if k == 0 else v_f)[...]
                v_half = v_old.astype(bf16)

                def pick(new, old):
                    if k == 0:
                        return new
                    return jnp.where(jnp.full(new.shape, count, jnp.int32) > k, new, old)

                grad_v = jnp.zeros((items, rank), f32)
                for s in starts:
                    rows = pl.ds(s, CHUNK)
                    u_half = u_b[rows, :]
                    approx = lax.dot_general(u_half, v_half, (((1,), (1,)), ((), ())), preferred_element_type=f32)
                    err = jnp.where(m_buf[q, rows, :] != 0, approx - r_buf[q, rows, :], 0.0).astype(bf16)
                    e_b[rows, :] = err
                    grad_v += lax.dot_general(err, u_half, (((0,), (0,)), ((), ())), preferred_element_type=f32)
                v_new = pick(keep * v_old - step_size * grad_v, v_old)
                if k < STEPS_MAX - 1:
                    v_f[...] = v_new
                else:
                    v_send[t] = v_new
                    hop_copy(t).start()

                for s in starts:
                    rows = pl.ds(s, CHUNK)
                    grad_u = jnp.dot(e_b[rows, :], v_half, preferred_element_type=f32)
                    u_old = u_f[rows, :]
                    u_new = pick(keep * u_old - step_size * grad_u, u_old)
                    u_f[rows, :] = u_new
                    u_b[rows, :] = u_new.astype(bf16)
            return carry

        lax.fori_loop(0, hops, sub_epoch, 0)
        u_back = pltpu.make_async_copy(u_f, u_out, out_sem.at[0])
        u_back.start()
        pltpu.make_async_copy(v_slot.at[hops], v_slot.at[hops], recv_sem.at[hops]).wait()
        v_back = pltpu.make_async_copy(v_slot.at[hops], v_out, out_sem.at[1])
        v_back.start()
        for t in range(hops):
            hop_copy(t).wait_send()
        u_back.wait()
        v_back.wait()

    return kernel


def solution(mesh):
    n = mesh.shape["shard"]
    row_spec = P(("rep", "shard"), None)
    hops = EPOCHS * n

    def local_run(ratings, obs_mask, step_counts, user_init, item_init):
        users, rank = user_init.shape
        items = item_init.shape[0]
        f32, bf16 = jnp.float32, jnp.bfloat16
        dma = pltpu.SemaphoreType.DMA
        hbm = pl.BlockSpec(memory_space=pl.ANY)
        return pl.pallas_call(
            make_kernel(n, users, items, rank),
            out_shape=(jax.ShapeDtypeStruct((users, rank), f32), jax.ShapeDtypeStruct((items, rank), f32)),
            in_specs=[pl.BlockSpec(memory_space=pltpu.SMEM), hbm, hbm, hbm, hbm],
            out_specs=(hbm, hbm),
            scratch_shapes=[
                pltpu.VMEM((n, users, items), f32),
                pltpu.VMEM((n, users, items), jnp.int32),
                pltpu.VMEM((users, rank), f32),
                pltpu.VMEM((users, rank), bf16),
                pltpu.VMEM((hops + 1, items, rank), f32),
                pltpu.VMEM((hops, items, rank), f32),
                pltpu.VMEM((items, rank), f32),
                pltpu.VMEM((users, items), bf16),
                dma((n,)), dma((n,)), dma, dma((hops + 1,)), dma((hops,)), dma((2,)),
            ],
            compiler_params=pltpu.CompilerParams(collective_id=0, has_side_effects=True),
            name="dsgd",
        )(step_counts, ratings, obs_mask, user_init, item_init)

    return jax.shard_map(local_run, mesh=mesh, in_specs=(row_spec,) * 5, out_specs=(row_spec, row_spec), check_vma=False)
```

```python
import math
import jax
import jax.numpy as jnp
from jax import lax
from jax.experimental import pallas as pl
from jax.experimental.pallas import tpu as pltpu
from jax.sharding import PartitionSpec as P

EPOCHS = 2
STEPS_MAX = 4
CHUNK = 128


def make_kernel(n, users, items, rank):
    step_size = 0.4 * math.sqrt(rank) / (users + rank)
    decay = 0.1 * items / math.sqrt(rank)
    keep = 1.0 - step_size * decay
    hops = EPOCHS * n
    bf16, f32 = jnp.bfloat16, jnp.float32
    starts = range(0, users, CHUNK)

    def kernel(cnt_hbm, r_hbm, m_hbm, u_hbm, v_hbm, u_f, v_out,
               cnt, r_buf, m_buf, u_b, v_slot, v_send, v_f, e_b,
               r_sem, m_sem, u_sem, cnt_sem, recv_sem, send_sem):
        me = lax.axis_index("shard")
        left, right = lax.rem(me + n - 1, n), lax.rem(me + 1, n)

        barrier = pltpu.get_barrier_semaphore()
        for peer in (left, right):
            pl.semaphore_signal(barrier, inc=1, device_id={"shard": peer}, device_id_type=pl.DeviceIdType.MESH)

        def block_copy(kind, q):
            src, dst, sem = ((r_hbm, r_buf, r_sem), (m_hbm, m_buf, m_sem))[kind]
            col = pl.multiple_of(lax.rem(me + q, n) * items, items)
            return pltpu.make_async_copy(src.at[:, pl.ds(col, items)], dst.at[q], sem.at[q])

        u_in = pltpu.make_async_copy(u_hbm, u_f, u_sem)
        v_in = pltpu.make_async_copy(v_hbm, v_slot.at[0], recv_sem.at[0])
        cnt_in = pltpu.make_async_copy(cnt_hbm, cnt, cnt_sem)
        u_in.start()
        v_in.start()
        cnt_in.start()
        for q in range(n):
            block_copy(0, q).start()
            block_copy(1, q).start()
        u_in.wait()
        for s in starts:
            u_b[pl.ds(s, CHUNK), :] = u_f[pl.ds(s, CHUNK), :].astype(bf16)
        v_in.wait()
        cnt_in.wait()
        pl.semaphore_wait(barrier, 2)

        def hop_copy(t):
            return pltpu.make_async_remote_copy(
                src_ref=v_send.at[t], dst_ref=v_slot.at[t + 1],
                send_sem=send_sem.at[t], recv_sem=recv_sem.at[t + 1],
                device_id={"shard": left}, device_id_type=pl.DeviceIdType.MESH)

        def sub_epoch(t, carry):
            q = lax.rem(t, n)
            count = cnt[0, lax.rem(me + t, n)]

            @pl.when(t < n)
            def _():
                block_copy(0, t).wait()
                block_copy(1, t).wait()

            @pl.when(t > 0)
            def _():
                pltpu.make_async_copy(v_slot.at[t], v_slot.at[t], recv_sem.at[t]).wait()

            for k in range(STEPS_MAX):
                v_old = (v_slot.at[t] if k == 0 else v_f)[...]
                v_half = v_old.astype(bf16)

                def pick(new, old):
                    if k == 0:
                        return new
                    return jnp.where(jnp.full(new.shape, count, jnp.int32) > k, new, old)

                grad_v = jnp.zeros((items, rank), f32)
                for s in starts:
                    rows = pl.ds(s, CHUNK)
                    u_half = u_b[rows, :]
                    approx = lax.dot_general(u_half, v_half, (((1,), (1,)), ((), ())), preferred_element_type=f32)
                    err = jnp.where(m_buf[q, rows, :] != 0, approx - r_buf[q, rows, :], 0.0).astype(bf16)
                    e_b[rows, :] = err
                    grad_v += lax.dot_general(err, u_half, (((0,), (0,)), ((), ())), preferred_element_type=f32)
                v_new = pick(keep * v_old - step_size * grad_v, v_old)
                if k < STEPS_MAX - 1:
                    v_f[...] = v_new
                else:
                    v_send[t] = v_new
                    hop_copy(t).start()

                for s in starts:
                    rows = pl.ds(s, CHUNK)
                    grad_u = jnp.dot(e_b[rows, :], v_half, preferred_element_type=f32)
                    u_old = u_f[rows, :]
                    u_new = pick(keep * u_old - step_size * grad_u, u_old)
                    u_f[rows, :] = u_new
                    u_b[rows, :] = u_new.astype(bf16)
            return carry

        lax.fori_loop(0, hops, sub_epoch, 0)
        pltpu.make_async_copy(v_slot.at[hops], v_slot.at[hops], recv_sem.at[hops]).wait()
        v_out[...] = v_slot[hops]
        for t in range(hops):
            hop_copy(t).wait_send()

    return kernel


def solution(mesh):
    n = mesh.shape["shard"]
    row_spec = P(("rep", "shard"), None)
    hops = EPOCHS * n

    def local_run(ratings, obs_mask, step_counts, user_init, item_init):
        users, rank = user_init.shape
        items = item_init.shape[0]
        f32, bf16 = jnp.float32, jnp.bfloat16
        dma = pltpu.SemaphoreType.DMA
        hbm = pl.BlockSpec(memory_space=pl.ANY)
        vmem = pl.BlockSpec(memory_space=pltpu.VMEM)
        return pl.pallas_call(
            make_kernel(n, users, items, rank),
            out_shape=(pltpu.VMEM((users, rank), f32), pltpu.VMEM((items, rank), f32)),
            in_specs=[hbm, hbm, hbm, hbm, hbm],
            out_specs=(vmem, vmem),
            scratch_shapes=[
                pltpu.SMEM((1, n), jnp.int32),
                pltpu.VMEM((n, users, items), f32),
                pltpu.VMEM((n, users, items), jnp.int32),
                pltpu.VMEM((users, rank), bf16),
                pltpu.VMEM((hops + 1, items, rank), f32),
                pltpu.VMEM((hops, items, rank), f32),
                pltpu.VMEM((items, rank), f32),
                pltpu.VMEM((users, items), bf16),
                dma((n,)), dma((n,)), dma, dma, dma((hops + 1,)), dma((hops,)),
            ],
            compiler_params=pltpu.CompilerParams(collective_id=0, has_side_effects=True),
            name="dsgd",
        )(step_counts, ratings, obs_mask, user_init, item_init)

    return jax.shard_map(local_run, mesh=mesh, in_specs=(row_spec,) * 5, out_specs=(row_spec, row_spec), check_vma=False)
```

```python
import math
import jax
import jax.numpy as jnp
from jax import lax
from jax.experimental import pallas as pl
from jax.experimental.pallas import tpu as pltpu
from jax.sharding import PartitionSpec as P

EPOCHS = 2
STEPS_MAX = 4
CHUNK = 320


def make_kernel(n, users, items, rank):
    step_size = 0.4 * math.sqrt(rank) / (users + rank)
    decay = 0.1 * items / math.sqrt(rank)
    keep = 1.0 - step_size * decay
    hops = EPOCHS * n
    bf16, f32 = jnp.bfloat16, jnp.float32
    starts = range(0, users, CHUNK)

    def kernel(cnt_hbm, r_hbm, m_hbm, u_hbm, v_hbm, u_f, v_out,
               cnt, r_buf, m_buf, u_b, v_slot, v_send, v_f, e_b,
               r_sem, m_sem, u_sem, cnt_sem, recv_sem, send_sem):
        me = lax.axis_index("shard")
        left, right = lax.rem(me + n - 1, n), lax.rem(me + 1, n)

        barrier = pltpu.get_barrier_semaphore()
        for peer in (left, right):
            pl.semaphore_signal(barrier, inc=1, device_id={"shard": peer}, device_id_type=pl.DeviceIdType.MESH)

        def block_copy(kind, q):
            src, dst, sem = ((r_hbm, r_buf, r_sem), (m_hbm, m_buf, m_sem))[kind]
            col = pl.multiple_of(lax.rem(me + q, n) * items, items)
            return pltpu.make_async_copy(src.at[:, pl.ds(col, items)], dst.at[q], sem.at[q])

        u_in = pltpu.make_async_copy(u_hbm, u_f, u_sem)
        v_in = pltpu.make_async_copy(v_hbm, v_slot.at[0], recv_sem.at[0])
        cnt_in = pltpu.make_async_copy(cnt_hbm, cnt, cnt_sem)
        u_in.start()
        v_in.start()
        cnt_in.start()
        for q in range(n):
            block_copy(0, q).start()
            block_copy(1, q).start()
        u_in.wait()
        for s in starts:
            u_b[pl.ds(s, CHUNK), :] = u_f[pl.ds(s, CHUNK), :].astype(bf16)
        v_in.wait()
        cnt_in.wait()
        pl.semaphore_wait(barrier, 2)

        def hop_copy(t):
            return pltpu.make_async_remote_copy(
                src_ref=v_send.at[t], dst_ref=v_slot.at[t + 1],
                send_sem=send_sem.at[t], recv_sem=recv_sem.at[t + 1],
                device_id={"shard": left}, device_id_type=pl.DeviceIdType.MESH)

        def sub_epoch(t, carry):
            q = lax.rem(t, n)
            count = cnt[0, lax.rem(me + t, n)]

            @pl.when(t < n)
            def _():
                block_copy(0, t).wait()
                block_copy(1, t).wait()

            @pl.when(t > 0)
            def _():
                pltpu.make_async_copy(v_slot.at[t], v_slot.at[t], recv_sem.at[t]).wait()

            for k in range(STEPS_MAX):
                v_old = (v_slot.at[t] if k == 0 else v_f)[...]
                v_half = v_old.astype(bf16)

                def pick(new, old):
                    if k == 0:
                        return new
                    return jnp.where(jnp.full(new.shape, count, jnp.int32) > k, new, old)

                grad_v = jnp.zeros((items, rank), f32)
                for s in starts:
                    rows = pl.ds(s, CHUNK)
                    u_half = u_b[rows, :]
                    approx = lax.dot_general(u_half, v_half, (((1,), (1,)), ((), ())), preferred_element_type=f32)
                    err = jnp.where(m_buf[q, rows, :] != 0, approx - r_buf[q, rows, :], 0.0).astype(bf16)
                    e_b[rows, :] = err
                    grad_v += lax.dot_general(err, u_half, (((0,), (0,)), ((), ())), preferred_element_type=f32)
                v_new = pick(keep * v_old - step_size * grad_v, v_old)
                if k < STEPS_MAX - 1:
                    v_f[...] = v_new
                else:
                    v_send[t] = v_new
                    hop_copy(t).start()

                for s in starts:
                    rows = pl.ds(s, CHUNK)
                    grad_u = jnp.dot(e_b[rows, :], v_half, preferred_element_type=f32)
                    u_old = u_f[rows, :]
                    u_new = pick(keep * u_old - step_size * grad_u, u_old)
                    u_f[rows, :] = u_new
                    u_b[rows, :] = u_new.astype(bf16)
            return carry

        lax.fori_loop(0, hops, sub_epoch, 0)
        pltpu.make_async_copy(v_slot.at[hops], v_slot.at[hops], recv_sem.at[hops]).wait()
        v_out[...] = v_slot[hops]
        for t in range(hops):
            hop_copy(t).wait_send()

    return kernel


def solution(mesh):
    n = mesh.shape["shard"]
    row_spec = P(("rep", "shard"), None)
    hops = EPOCHS * n

    def local_run(ratings, obs_mask, step_counts, user_init, item_init):
        users, rank = user_init.shape
        items = item_init.shape[0]
        f32, bf16 = jnp.float32, jnp.bfloat16
        dma = pltpu.SemaphoreType.DMA
        hbm = pl.BlockSpec(memory_space=pl.ANY)
        vmem = pl.BlockSpec(memory_space=pltpu.VMEM)
        return pl.pallas_call(
            make_kernel(n, users, items, rank),
            out_shape=(pltpu.VMEM((users, rank), f32), pltpu.VMEM((items, rank), f32)),
            in_specs=[hbm, hbm, hbm, hbm, hbm],
            out_specs=(vmem, vmem),
            scratch_shapes=[
                pltpu.SMEM((1, n), jnp.int32),
                pltpu.VMEM((n, users, items), f32),
                pltpu.VMEM((n, users, items), jnp.int32),
                pltpu.VMEM((users, rank), bf16),
                pltpu.VMEM((hops + 1, items, rank), f32),
                pltpu.VMEM((hops, items, rank), f32),
                pltpu.VMEM((items, rank), f32),
                pltpu.VMEM((users, items), bf16),
                dma((n,)), dma((n,)), dma, dma, dma((hops + 1,)), dma((hops,)),
            ],
            compiler_params=pltpu.CompilerParams(collective_id=0, has_side_effects=True),
            name="dsgd",
        )(step_counts, ratings, obs_mask, user_init, item_init)

    return jax.shard_map(local_run, mesh=mesh, in_specs=(row_spec,) * 5, out_specs=(row_spec, row_spec), check_vma=False)
```

```python
import math
import jax
import jax.numpy as jnp
from jax import lax
from jax.experimental import pallas as pl
from jax.experimental.pallas import tpu as pltpu
from jax.sharding import PartitionSpec as P

EPOCHS = 2
STEPS_MAX = 4
TILE = 256


def make_kernel(n, users, items, rank):
    step_size = 0.4 * math.sqrt(rank) / (users + rank)
    decay = 0.1 * items / math.sqrt(rank)
    keep = 1.0 - step_size * decay
    hops = EPOCHS * n
    bf16, f32 = jnp.bfloat16, jnp.float32
    tiles = [(s, min(TILE, users - s)) for s in range(0, users, TILE)]

    def nn(a, b):
        return lax.dot_general(a, b, (((1,), (0,)), ((), ())), preferred_element_type=f32)

    def nt(a, b):
        return lax.dot_general(a, b, (((1,), (1,)), ((), ())), preferred_element_type=f32)

    def split(w, rows):
        return [(0, rows)] if w == TILE else [(0, rows // 2), (rows // 2, rows // 2)]

    def kernel(cnt_hbm, r_hbm, m_hbm, u_hbm, v_hbm, u_out, v_out,
               cnt, r_buf, m_buf, r_t, m_t, ut_f, ut_b, v_slot, v_send, v_f, e_b, vt_b,
               r_sem, m_sem, u_sem, cnt_sem, recv_sem, send_sem):
        me = lax.axis_index("shard")
        left, right = lax.rem(me + n - 1, n), lax.rem(me + 1, n)

        barrier = pltpu.get_barrier_semaphore()
        for peer in (left, right):
            pl.semaphore_signal(barrier, inc=1, device_id={"shard": peer}, device_id_type=pl.DeviceIdType.MESH)

        def block_copy(kind, q):
            src, dst, sem = ((r_hbm, r_buf, r_sem), (m_hbm, m_buf, m_sem))[kind]
            col = pl.multiple_of(lax.rem(me + q, n) * items, items)
            return pltpu.make_async_copy(src.at[:, pl.ds(col, items)], dst.at[q], sem.at[q])

        u_in = pltpu.make_async_copy(u_hbm, u_out, u_sem)
        v_in = pltpu.make_async_copy(v_hbm, v_slot.at[0], recv_sem.at[0])
        cnt_in = pltpu.make_async_copy(cnt_hbm, cnt, cnt_sem)
        u_in.start()
        v_in.start()
        cnt_in.start()
        for q in range(n):
            block_copy(0, q).start()
            block_copy(1, q).start()

        def flip_block(q):
            block_copy(0, q).wait()
            block_copy(1, q).wait()
            for s in range(0, users, 128):
                r_t[q, :, pl.ds(s, 128)] = r_buf[q, pl.ds(s, 128), :].T
                m_t[q, :, pl.ds(s, 128)] = m_buf[q, pl.ds(s, 128), :].astype(f32).T.astype(bf16)

        u_in.wait()
        for s in range(0, users, 128):
            flipped = u_out[pl.ds(s, 128), :].T
            ut_f[:, pl.ds(s, 128)] = flipped
            ut_b[:, pl.ds(s, 128)] = flipped.astype(bf16)
        flip_block(0)
        v_in.wait()
        cnt_in.wait()
        pl.semaphore_wait(barrier, 2)

        def hop_copy(t):
            return pltpu.make_async_remote_copy(
                src_ref=v_send.at[t], dst_ref=v_slot.at[t + 1],
                send_sem=send_sem.at[t], recv_sem=recv_sem.at[t + 1],
                device_id={"shard": left}, device_id_type=pl.DeviceIdType.MESH)

        def sub_epoch(t, carry):
            q = lax.rem(t, n)
            count = cnt[0, lax.rem(me + t, n)]

            @pl.when(t > 0)
            def _():
                pltpu.make_async_copy(v_slot.at[t], v_slot.at[t], recv_sem.at[t]).wait()

            for k in range(STEPS_MAX):
                v_old = (v_slot.at[t] if k == 0 else v_f)[...]
                v_half = v_old.astype(bf16)
                vt_b[...] = v_half.T

                def pick(new, old):
                    if k == 0:
                        return new
                    return jnp.where(jnp.full(new.shape, count, jnp.int32) > k, new, old)

                for s, w in tiles:
                    cols = pl.ds(s, w)
                    for a, h in split(w, items):
                        approx = nn(v_half[a:a + h], ut_b[:, cols])
                        err = (approx - r_t[q, pl.ds(a, h), cols]).astype(bf16)
                        seen = m_t[q, pl.ds(a, h), cols] != 0
                        e_b[pl.ds(a, h), cols] = jnp.where(seen, err, jnp.zeros_like(err))
                halves = []
                for a, h in ((0, items // 2), (items // 2, items // 2)):
                    halves.append(keep * v_old[a:a + h])
                for s, w in tiles:
                    cols = pl.ds(s, w)
                    if w == TILE:
                        g = step_size * nt(e_b[:, cols], ut_b[:, cols])
                        halves = [halves[0] - g[:items // 2], halves[1] - g[items // 2:]]
                    else:
                        halves = [x - step_size * nt(e_b[pl.ds(i * items // 2, items // 2), cols], ut_b[:, cols])
                                  for i, x in enumerate(halves)]
                v_new = pick(jnp.concatenate(halves, axis=0), v_old)
                if k < STEPS_MAX - 1:
                    v_f[...] = v_new
                else:
                    v_send[t] = v_new
                    hop_copy(t).start()

                for s, w in tiles:
                    cols = pl.ds(s, w)
                    for a, h in split(w, rank):
                        rows = pl.ds(a, h)
                        grad = nn(vt_b[rows, :], e_b[:, cols])
                        u_old = ut_f[rows, cols]
                        u_new = pick(keep * u_old - step_size * grad, u_old)
                        ut_f[rows, cols] = u_new
                        ut_b[rows, cols] = u_new.astype(bf16)

            @pl.when(t + 1 < n)
            def _():
                flip_block(t + 1)

            return carry

        lax.fori_loop(0, hops, sub_epoch, 0)
        for s in range(0, users, 128):
            u_out[pl.ds(s, 128), :] = ut_f[:, pl.ds(s, 128)].T
        pltpu.make_async_copy(v_slot.at[hops], v_slot.at[hops], recv_sem.at[hops]).wait()
        v_out[...] = v_slot[hops]
        for t in range(hops):
            hop_copy(t).wait_send()

    return kernel


def solution(mesh):
    n = mesh.shape["shard"]
    row_spec = P(("rep", "shard"), None)
    hops = EPOCHS * n

    def local_run(ratings, obs_mask, step_counts, user_init, item_init):
        users, rank = user_init.shape
        items = item_init.shape[0]
        f32, bf16 = jnp.float32, jnp.bfloat16
        dma = pltpu.SemaphoreType.DMA
        hbm = pl.BlockSpec(memory_space=pl.ANY)
        vmem = pl.BlockSpec(memory_space=pltpu.VMEM)
        return pl.pallas_call(
            make_kernel(n, users, items, rank),
            out_shape=(pltpu.VMEM((users, rank), f32), pltpu.VMEM((items, rank), f32)),
            in_specs=[hbm, hbm, hbm, hbm, hbm],
            out_specs=(vmem, vmem),
            scratch_shapes=[
                pltpu.SMEM((1, n), jnp.int32),
                pltpu.VMEM((n, users, items), f32),
                pltpu.VMEM((n, users, items), jnp.int32),
                pltpu.VMEM((n, items, users), f32),
                pltpu.VMEM((n, items, users), bf16),
                pltpu.VMEM((rank, users), f32),
                pltpu.VMEM((rank, users), bf16),
                pltpu.VMEM((hops + 1, items, rank), f32),
                pltpu.VMEM((hops, items, rank), f32),
                pltpu.VMEM((items, rank), f32),
                pltpu.VMEM((items, users), bf16),
                pltpu.VMEM((rank, items), bf16),
                dma((n,)), dma((n,)), dma, dma, dma((hops + 1,)), dma((hops,)),
            ],
            compiler_params=pltpu.CompilerParams(collective_id=0, has_side_effects=True),
            name="dsgd",
        )(step_counts, ratings, obs_mask, user_init, item_init)

    return jax.shard_map(local_run, mesh=mesh, in_specs=(row_spec,) * 5, out_specs=(row_spec, row_spec), check_vma=False)
```

```python
import math
import jax
import jax.numpy as jnp
from jax import lax
from jax.experimental import pallas as pl
from jax.experimental.pallas import tpu as pltpu
from jax.sharding import PartitionSpec as P

EPOCHS = 2
STEPS_MAX = 4
TILE = 256


def make_kernel(n, users, items, rank):
    step_size = 0.4 * math.sqrt(rank) / (users + rank)
    decay = 0.1 * items / math.sqrt(rank)
    keep = 1.0 - step_size * decay
    hops = EPOCHS * n
    bf16, f32 = jnp.bfloat16, jnp.float32
    tiles = [(s, min(TILE, users - s)) for s in range(0, users, TILE)]

    def nn(a, b):
        return lax.dot_general(a, b, (((1,), (0,)), ((), ())), preferred_element_type=f32)

    def nt(a, b):
        return lax.dot_general(a, b, (((1,), (1,)), ((), ())), preferred_element_type=f32)

    def split(w, rows):
        return [(0, rows)] if w == TILE else [(0, rows // 2), (rows // 2, rows // 2)]

    def kernel(cnt_hbm, r_hbm, m_hbm, u_hbm, v_hbm, u_out, v_out,
               cnt, r_buf, m_buf, r_t, m_t, ut_f, ut_b, v_slot, v_send, v_f, e_b, vt_b,
               r_sem, m_sem, u_sem, cnt_sem, recv_sem, send_sem):
        me = lax.axis_index("shard")
        left, right = lax.rem(me + n - 1, n), lax.rem(me + 1, n)

        barrier = pltpu.get_barrier_semaphore()
        for peer in (left, right):
            pl.semaphore_signal(barrier, inc=1, device_id={"shard": peer}, device_id_type=pl.DeviceIdType.MESH)

        def block_copy(kind, q):
            src, dst, sem = ((r_hbm, r_buf, r_sem), (m_hbm, m_buf, m_sem))[kind]
            col = pl.multiple_of(lax.rem(me + q, n) * items, items)
            return pltpu.make_async_copy(src.at[:, pl.ds(col, items)], dst.at[q], sem.at[q])

        u_in = pltpu.make_async_copy(u_hbm, u_out, u_sem)
        v_in = pltpu.make_async_copy(v_hbm, v_slot.at[0], recv_sem.at[0])
        cnt_in = pltpu.make_async_copy(cnt_hbm, cnt, cnt_sem)
        u_in.start()
        v_in.start()
        cnt_in.start()
        block_copy(0, 0).start()
        block_copy(1, 0).start()

        def flip_block(q):
            block_copy(0, q).wait()
            block_copy(1, q).wait()
            for s in range(0, users, 128):
                r_t[q, :, pl.ds(s, 128)] = r_buf[q, pl.ds(s, 128), :].T
                m_t[q, :, pl.ds(s, 128)] = m_buf[q, pl.ds(s, 128), :].astype(f32).T.astype(bf16)

        u_in.wait()
        for s in range(0, users, 128):
            flipped = u_out[pl.ds(s, 128), :].T
            ut_f[:, pl.ds(s, 128)] = flipped
            ut_b[:, pl.ds(s, 128)] = flipped.astype(bf16)
        flip_block(0)
        for q in range(1, n):
            block_copy(0, q).start()
            block_copy(1, q).start()
        v_in.wait()
        cnt_in.wait()
        pl.semaphore_wait(barrier, 2)

        def hop_copy(t):
            return pltpu.make_async_remote_copy(
                src_ref=v_send.at[t], dst_ref=v_slot.at[t + 1],
                send_sem=send_sem.at[t], recv_sem=recv_sem.at[t + 1],
                device_id={"shard": left}, device_id_type=pl.DeviceIdType.MESH)

        def sub_epoch(t, carry):
            q = lax.rem(t, n)
            count = cnt[0, lax.rem(me + t, n)]

            @pl.when(t > 0)
            def _():
                pltpu.make_async_copy(v_slot.at[t], v_slot.at[t], recv_sem.at[t]).wait()

            for k in range(STEPS_MAX):
                v_old = (v_slot.at[t] if k == 0 else v_f)[...]
                v_half = v_old.astype(bf16)
                if k == 0:
                    limit, keep_k = 0.5, keep
                    vt_b[...] = v_half.T
                else:
                    live = count > k
                    limit = jnp.where(live, 0.5, 2.0)
                    keep_k = jnp.where(live, keep, 1.0)
                    v_live = jnp.where(jnp.full(v_half.shape, count, jnp.int32) > k, v_old, 0.0).astype(bf16)
                    vt_b[...] = v_live.T

                def pick(new, old):
                    if k == 0:
                        return new
                    return jnp.where(jnp.full(new.shape, count, jnp.int32) > k, new, old)

                for s, w in tiles:
                    cols = pl.ds(s, w)
                    for a, h in split(w, items):
                        approx = nn(v_half[a:a + h], ut_b[:, cols])
                        err = (approx - r_t[q, pl.ds(a, h), cols]).astype(bf16)
                        seen = m_t[q, pl.ds(a, h), cols] > jnp.full((h, w), limit, f32).astype(bf16)
                        e_b[pl.ds(a, h), cols] = jnp.where(seen, err, jnp.zeros_like(err))
                half = items // 2
                parts = [keep * v_old[i * half:(i + 1) * half] for i in range(2)]

                def item_grad(s, w):
                    cols = pl.ds(s, w)
                    if w == TILE:
                        g = step_size * nt(e_b[:, cols], ut_b[:, cols])
                        for i in range(2):
                            parts[i] = parts[i] - g[i * half:(i + 1) * half]
                    else:
                        for i in range(2):
                            parts[i] = parts[i] - step_size * nt(e_b[pl.ds(i * half, half), cols], ut_b[:, cols])

                def item_update():
                    v_new = pick(jnp.concatenate(parts, axis=0), v_old)
                    if k < STEPS_MAX - 1:
                        v_f[...] = v_new
                    else:
                        v_send[t] = v_new
                        hop_copy(t).start()

                def user_update(s, w):
                    cols = pl.ds(s, w)
                    for a, h in split(w, rank):
                        rows = pl.ds(a, h)
                        grad = nn(vt_b[rows, :], e_b[:, cols])
                        u_new = keep_k * ut_f[rows, cols] - step_size * grad
                        ut_f[rows, cols] = u_new
                        ut_b[rows, cols] = u_new.astype(bf16)

                wide = [x for x in tiles if x[1] == TILE]
                narrow = [x for x in tiles if x[1] < TILE]
                if k < STEPS_MAX - 1:
                    order = [(item_grad, wide), (user_update, wide), (item_grad, narrow), (item_update, None), (user_update, narrow)]
                else:
                    order = [(item_grad, wide), (item_grad, narrow), (item_update, None), (user_update, wide), (user_update, narrow)]
                for piece, group in order:
                    if group is None:
                        piece()
                    else:
                        for x in group:
                            piece(*x)

            @pl.when(t + 1 < n)
            def _():
                flip_block(t + 1)

            return carry

        lax.fori_loop(0, hops, sub_epoch, 0)
        for s in range(0, users, 128):
            u_out[pl.ds(s, 128), :] = ut_f[:, pl.ds(s, 128)].T
        pltpu.make_async_copy(v_slot.at[hops], v_slot.at[hops], recv_sem.at[hops]).wait()
        v_out[...] = v_slot[hops]
        for t in range(hops):
            hop_copy(t).wait_send()

    return kernel


def solution(mesh):
    n = mesh.shape["shard"]
    row_spec = P(("rep", "shard"), None)
    hops = EPOCHS * n

    def local_run(ratings, obs_mask, step_counts, user_init, item_init):
        users, rank = user_init.shape
        items = item_init.shape[0]
        f32, bf16 = jnp.float32, jnp.bfloat16
        dma = pltpu.SemaphoreType.DMA
        hbm = pl.BlockSpec(memory_space=pl.ANY)
        vmem = pl.BlockSpec(memory_space=pltpu.VMEM)
        return pl.pallas_call(
            make_kernel(n, users, items, rank),
            out_shape=(pltpu.VMEM((users, rank), f32), pltpu.VMEM((items, rank), f32)),
            in_specs=[hbm, hbm, hbm, hbm, hbm],
            out_specs=(vmem, vmem),
            scratch_shapes=[
                pltpu.SMEM((1, n), jnp.int32),
                pltpu.VMEM((n, users, items), f32),
                pltpu.VMEM((n, users, items), jnp.int32),
                pltpu.VMEM((n, items, users), f32),
                pltpu.VMEM((n, items, users), bf16),
                pltpu.VMEM((rank, users), f32),
                pltpu.VMEM((rank, users), bf16),
                pltpu.VMEM((hops + 1, items, rank), f32),
                pltpu.VMEM((hops, items, rank), f32),
                pltpu.VMEM((items, rank), f32),
                pltpu.VMEM((items, users), bf16),
                pltpu.VMEM((rank, items), bf16),
                dma((n,)), dma((n,)), dma, dma, dma((hops + 1,)), dma((hops,)),
            ],
            compiler_params=pltpu.CompilerParams(collective_id=0, has_side_effects=True),
            name="dsgd",
        )(step_counts, ratings, obs_mask, user_init, item_init)

    return jax.shard_map(local_run, mesh=mesh, in_specs=(row_spec,) * 5, out_specs=(row_spec, row_spec), check_vma=False)
```

```python
import math
import jax
import jax.numpy as jnp
from jax import lax
from jax.experimental import pallas as pl
from jax.experimental.pallas import tpu as pltpu
from jax.sharding import PartitionSpec as P

EPOCHS = 2
STEPS_MAX = 4
TILE = 256


def make_kernel(n, users, items, rank):
    step_size = 0.4 * math.sqrt(rank) / (users + rank)
    decay = 0.1 * items / math.sqrt(rank)
    keep = 1.0 - step_size * decay
    hops = EPOCHS * n
    bf16, f32 = jnp.bfloat16, jnp.float32
    tiles = [(s, min(TILE, users - s)) for s in range(0, users, TILE)]

    def nn(a, b):
        return lax.dot_general(a, b, (((1,), (0,)), ((), ())), preferred_element_type=f32)

    def nt(a, b):
        return lax.dot_general(a, b, (((1,), (1,)), ((), ())), preferred_element_type=f32)

    def split(w, rows):
        return [(0, rows)] if w == TILE else [(0, rows // 2), (rows // 2, rows // 2)]

    def kernel(cnt_hbm, r_hbm, m_hbm, u_hbm, v_hbm, u_out, v_out,
               cnt, r_buf, m_buf, r_t, m_t, ut_f, ut_b, v_slot, v_send, v_f, e_b, vt_b,
               r_sem, m_sem, u_sem, cnt_sem, recv_sem, send_sem):
        me = lax.axis_index("shard")
        left, right = lax.rem(me + n - 1, n), lax.rem(me + 1, n)

        barrier = pltpu.get_barrier_semaphore()
        for peer in (left, right):
            pl.semaphore_signal(barrier, inc=1, device_id={"shard": peer}, device_id_type=pl.DeviceIdType.MESH)

        def block_copy(kind, q):
            src, dst, sem = ((r_hbm, r_buf, r_sem), (m_hbm, m_buf, m_sem))[kind]
            col = pl.multiple_of(lax.rem(me + q, n) * items, items)
            return pltpu.make_async_copy(src.at[:, pl.ds(col, items)], dst.at[q], sem.at[q])

        u_in = pltpu.make_async_copy(u_hbm, u_out, u_sem)
        v_in = pltpu.make_async_copy(v_hbm, v_slot.at[0], recv_sem.at[0])
        cnt_in = pltpu.make_async_copy(cnt_hbm, cnt, cnt_sem)
        u_in.start()
        v_in.start()
        cnt_in.start()
        block_copy(0, 0).start()
        block_copy(1, 0).start()

        def flip_block(q):
            block_copy(0, q).wait()
            block_copy(1, q).wait()
            for s in range(0, users, 128):
                r_t[q, :, pl.ds(s, 128)] = r_buf[q, pl.ds(s, 128), :].T
                m_t[q, :, pl.ds(s, 128)] = m_buf[q, pl.ds(s, 128), :].astype(f32).T.astype(bf16)

        u_in.wait()
        for s in range(0, users, 128):
            flipped = u_out[pl.ds(s, 128), :].T
            ut_f[:, pl.ds(s, 128)] = flipped
            ut_b[:, pl.ds(s, 128)] = flipped.astype(bf16)
        flip_block(0)
        for q in range(1, n):
            block_copy(0, q).start()
            block_copy(1, q).start()
        v_in.wait()
        cnt_in.wait()
        pl.semaphore_wait(barrier, 2)

        def hop_copy(t):
            return pltpu.make_async_remote_copy(
                src_ref=v_send.at[t], dst_ref=v_slot.at[t + 1],
                send_sem=send_sem.at[t], recv_sem=recv_sem.at[t + 1],
                device_id={"shard": left}, device_id_type=pl.DeviceIdType.MESH)

        def sub_epoch(t, carry):
            q = lax.rem(t, n)
            count = cnt[0, lax.rem(me + t, n)]

            @pl.when(t > 0)
            def _():
                pltpu.make_async_copy(v_slot.at[t], v_slot.at[t], recv_sem.at[t]).wait()

            for k in range(STEPS_MAX):
                v_old = (v_slot.at[t] if k == 0 else v_f)[...]
                v_half = v_old.astype(bf16)
                if k == 0:
                    limit, keep_k = 0.5, keep
                    vt_b[...] = v_half.T
                else:
                    live = count > k
                    limit = jnp.where(live, 0.5, 2.0)
                    keep_k = jnp.where(live, keep, 1.0)
                    v_live = jnp.where(jnp.full(v_half.shape, count, jnp.int32) > k, v_old, 0.0).astype(bf16)
                    vt_b[...] = v_live.T

                def pick(new, old):
                    if k == 0:
                        return new
                    return jnp.where(jnp.full(new.shape, count, jnp.int32) > k, new, old)

                for s, w in tiles:
                    cols = pl.ds(s, w)
                    for a, h in split(w, items):
                        approx = nn(v_half[a:a + h], ut_b[:, cols])
                        err = (approx - r_t[q, pl.ds(a, h), cols]).astype(bf16)
                        seen = m_t[q, pl.ds(a, h), cols] > jnp.full((h, w), limit, f32).astype(bf16)
                        e_b[pl.ds(a, h), cols] = jnp.where(seen, err, jnp.zeros_like(err))
                half = items // 2
                parts = [keep * v_old[i * half:(i + 1) * half] for i in range(2)]

                def item_grad(s, w):
                    cols = pl.ds(s, w)
                    if w == TILE:
                        g = step_size * nt(e_b[:, cols], ut_b[:, cols])
                        for i in range(2):
                            parts[i] = parts[i] - g[i * half:(i + 1) * half]
                    else:
                        for i in range(2):
                            parts[i] = parts[i] - step_size * nt(e_b[pl.ds(i * half, half), cols], ut_b[:, cols])

                def item_update():
                    v_new = pick(jnp.concatenate(parts, axis=0), v_old)
                    if k < STEPS_MAX - 1:
                        v_f[...] = v_new
                    else:
                        v_send[t] = v_new
                        hop_copy(t).start()

                def user_update(s, w):
                    cols = pl.ds(s, w)
                    for a, h in split(w, rank):
                        rows = pl.ds(a, h)
                        grad = nn(vt_b[rows, :], e_b[:, cols])
                        u_new = keep_k * ut_f[rows, cols] - step_size * grad
                        ut_f[rows, cols] = u_new
                        ut_b[rows, cols] = u_new.astype(bf16)

                wide = [x for x in tiles if x[1] == TILE]
                narrow = [x for x in tiles if x[1] < TILE]
                if k < STEPS_MAX - 1:
                    order = [(item_grad, wide), (user_update, wide), (item_grad, narrow), (item_update, None), (user_update, narrow)]
                else:
                    order = [(item_grad, wide), (item_grad, narrow), (item_update, None), (user_update, wide), (user_update, narrow)]
                for piece, group in order:
                    if group is None:
                        piece()
                    else:
                        for x in group:
                            piece(*x)

            @pl.when(t + 1 < n)
            def _():
                flip_block(t + 1)

            return carry

        lax.fori_loop(0, hops, sub_epoch, 0)
        for s in range(0, users, 128):
            u_out[pl.ds(s, 128), :] = ut_f[:, pl.ds(s, 128)].T
        pltpu.make_async_copy(v_slot.at[hops], v_slot.at[hops], recv_sem.at[hops]).wait()
        v_out[...] = v_slot[hops]
        for t in range(hops):
            hop_copy(t).wait_send()

    return kernel


def flush(u_vmem, v_vmem, u_out, v_out, sem):
    copies = [pltpu.make_async_copy(u_vmem, u_out, sem.at[0]), pltpu.make_async_copy(v_vmem, v_out, sem.at[1])]
    for copy in copies:
        copy.start()
    for copy in copies:
        copy.wait()


def solution(mesh):
    n = mesh.shape["shard"]
    row_spec = P(("rep", "shard"), None)
    hops = EPOCHS * n

    def local_run(ratings, obs_mask, step_counts, user_init, item_init):
        users, rank = user_init.shape
        items = item_init.shape[0]
        f32, bf16 = jnp.float32, jnp.bfloat16
        dma = pltpu.SemaphoreType.DMA
        hbm = pl.BlockSpec(memory_space=pl.ANY)
        vmem = pl.BlockSpec(memory_space=pltpu.VMEM)
        factors = pl.pallas_call(
            make_kernel(n, users, items, rank),
            out_shape=(pltpu.VMEM((users, rank), f32), pltpu.VMEM((items, rank), f32)),
            in_specs=[hbm, hbm, hbm, hbm, hbm],
            out_specs=(vmem, vmem),
            scratch_shapes=[
                pltpu.SMEM((1, n), jnp.int32),
                pltpu.VMEM((n, users, items), f32),
                pltpu.VMEM((n, users, items), jnp.int32),
                pltpu.VMEM((n, items, users), f32),
                pltpu.VMEM((n, items, users), bf16),
                pltpu.VMEM((rank, users), f32),
                pltpu.VMEM((rank, users), bf16),
                pltpu.VMEM((hops + 1, items, rank), f32),
                pltpu.VMEM((hops, items, rank), f32),
                pltpu.VMEM((items, rank), f32),
                pltpu.VMEM((items, users), bf16),
                pltpu.VMEM((rank, items), bf16),
                dma((n,)), dma((n,)), dma, dma, dma((hops + 1,)), dma((hops,)),
            ],
            compiler_params=pltpu.CompilerParams(collective_id=0, has_side_effects=True),
            name="dsgd",
        )(step_counts, ratings, obs_mask, user_init, item_init)
        return pl.pallas_call(
            flush,
            out_shape=(jax.ShapeDtypeStruct((users, rank), f32), jax.ShapeDtypeStruct((items, rank), f32)),
            in_specs=[vmem, vmem],
            out_specs=(hbm, hbm),
            scratch_shapes=[dma((2,))],
            compiler_params=pltpu.CompilerParams(vmem_limit_bytes=1 << 20),
            name="flush",
        )(*(pltpu.with_memory_space_constraint(x, pltpu.VMEM) for x in factors))

    return jax.shard_map(local_run, mesh=mesh, in_specs=(row_spec,) * 5, out_specs=(row_spec, row_spec), check_vma=False)
```

```python
import math
import jax
import jax.numpy as jnp
from jax import lax
from jax.experimental import pallas as pl
from jax.experimental.pallas import tpu as pltpu
from jax.sharding import PartitionSpec as P

EPOCHS = 2
STEPS_MAX = 4
TILE = 256
PIECES = 4


def make_kernel(n, users, items, rank):
    step_size = 0.4 * math.sqrt(rank) / (users + rank)
    decay = 0.1 * items / math.sqrt(rank)
    keep = 1.0 - step_size * decay
    hops = EPOCHS * n
    bf16, f32 = jnp.bfloat16, jnp.float32
    tiles = [(s, min(TILE, users - s)) for s in range(0, users, TILE)]

    def nn(a, b):
        return lax.dot_general(a, b, (((1,), (0,)), ((), ())), preferred_element_type=f32)

    def nt(a, b):
        return lax.dot_general(a, b, (((1,), (1,)), ((), ())), preferred_element_type=f32)

    def split(w, rows):
        return [(0, rows)] if w == TILE else [(0, rows // 2), (rows // 2, rows // 2)]

    def kernel(cnt_hbm, r_hbm, m_hbm, u_hbm, v_hbm, u_out, v_out,
               cnt, r_buf, m_buf, r_t, m_t, ut_f, ut_b, v_slot, v_send, v_f, e_b, vt_b,
               r_sem, m_sem, u_sem, v_sem, cnt_sem, recv_sem, send_sem):
        me = lax.axis_index("shard")
        left, right = lax.rem(me + n - 1, n), lax.rem(me + 1, n)

        barrier = pltpu.get_barrier_semaphore()
        for peer in (left, right):
            pl.semaphore_signal(barrier, inc=1, device_id={"shard": peer}, device_id_type=pl.DeviceIdType.MESH)

        def block_copy(kind, q):
            src, dst, sem = ((r_hbm, r_buf, r_sem), (m_hbm, m_buf, m_sem))[kind]
            col = pl.multiple_of(lax.rem(me + q, n) * items, items)
            return pltpu.make_async_copy(src.at[:, pl.ds(col, items)], dst.at[q], sem.at[q])

        u_in = pltpu.make_async_copy(u_hbm, u_out, u_sem)
        v_in = pltpu.make_async_copy(v_hbm, v_slot.at[0], v_sem)
        cnt_in = pltpu.make_async_copy(cnt_hbm, cnt, cnt_sem)
        u_in.start()
        v_in.start()
        cnt_in.start()
        block_copy(0, 0).start()
        block_copy(1, 0).start()

        def flip_block(q):
            block_copy(0, q).wait()
            block_copy(1, q).wait()
            for s in range(0, users, 128):
                r_t[q, :, pl.ds(s, 128)] = r_buf[q, pl.ds(s, 128), :].T
                m_t[q, :, pl.ds(s, 128)] = m_buf[q, pl.ds(s, 128), :].astype(f32).T.astype(bf16)

        u_in.wait()
        for s in range(0, users, 128):
            flipped = u_out[pl.ds(s, 128), :].T
            ut_f[:, pl.ds(s, 128)] = flipped
            ut_b[:, pl.ds(s, 128)] = flipped.astype(bf16)
        flip_block(0)
        for q in range(1, n):
            block_copy(0, q).start()
            block_copy(1, q).start()
        v_in.wait()
        cnt_in.wait()
        pl.semaphore_wait(barrier, 2)

        def hop_copy(t, i):
            rows = pl.ds(i * (items // PIECES), items // PIECES)
            return pltpu.make_async_remote_copy(
                src_ref=v_send.at[t, rows], dst_ref=v_slot.at[t + 1, rows],
                send_sem=send_sem.at[i, t], recv_sem=recv_sem.at[i, t],
                device_id={"shard": left}, device_id_type=pl.DeviceIdType.MESH)

        def sub_epoch(t, carry):
            q = lax.rem(t, n)
            count = cnt[0, lax.rem(me + t, n)]

            @pl.when(t > 0)
            def _():
                for i in range(PIECES):
                    hop_copy(t - 1, i).wait_recv()

            for k in range(STEPS_MAX):
                v_old = (v_slot.at[t] if k == 0 else v_f)[...]
                v_half = v_old.astype(bf16)
                if k == 0:
                    limit, keep_k = 0.5, keep
                    vt_b[...] = v_half.T
                else:
                    live = count > k
                    limit = jnp.where(live, 0.5, 2.0)
                    keep_k = jnp.where(live, keep, 1.0)
                    v_live = jnp.where(jnp.full(v_half.shape, count, jnp.int32) > k, v_old, 0.0).astype(bf16)
                    vt_b[...] = v_live.T

                def pick(new, old):
                    if k == 0:
                        return new
                    return jnp.where(jnp.full(new.shape, count, jnp.int32) > k, new, old)

                for s, w in tiles:
                    cols = pl.ds(s, w)
                    for a, h in split(w, items):
                        approx = nn(v_half[a:a + h], ut_b[:, cols])
                        err = (approx - r_t[q, pl.ds(a, h), cols]).astype(bf16)
                        seen = m_t[q, pl.ds(a, h), cols] > jnp.full((h, w), limit, f32).astype(bf16)
                        e_b[pl.ds(a, h), cols] = jnp.where(seen, err, jnp.zeros_like(err))
                half = items // 2
                parts = [keep * v_old[i * half:(i + 1) * half] for i in range(2)]

                def item_grad(s, w):
                    cols = pl.ds(s, w)
                    if w == TILE:
                        g = step_size * nt(e_b[:, cols], ut_b[:, cols])
                        for i in range(2):
                            parts[i] = parts[i] - g[i * half:(i + 1) * half]
                    else:
                        for i in range(2):
                            parts[i] = parts[i] - step_size * nt(e_b[pl.ds(i * half, half), cols], ut_b[:, cols])

                def item_update():
                    v_new = pick(jnp.concatenate(parts, axis=0), v_old)
                    if k < STEPS_MAX - 1:
                        v_f[...] = v_new
                    else:
                        for i in range(PIECES):
                            rows = items // PIECES
                            v_send[t, pl.ds(i * rows, rows), :] = v_new[i * rows:(i + 1) * rows]
                            hop_copy(t, i).start()

                def user_update(s, w):
                    cols = pl.ds(s, w)
                    for a, h in split(w, rank):
                        rows = pl.ds(a, h)
                        grad = nn(vt_b[rows, :], e_b[:, cols])
                        u_new = keep_k * ut_f[rows, cols] - step_size * grad
                        ut_f[rows, cols] = u_new
                        ut_b[rows, cols] = u_new.astype(bf16)

                wide = [x for x in tiles if x[1] == TILE]
                narrow = [x for x in tiles if x[1] < TILE]
                if k < STEPS_MAX - 1:
                    order = [(item_grad, wide), (user_update, wide), (item_grad, narrow), (item_update, None), (user_update, narrow)]
                else:
                    order = [(item_grad, wide), (item_grad, narrow), (item_update, None), (user_update, wide), (user_update, narrow)]
                for piece, group in order:
                    if group is None:
                        piece()
                    else:
                        for x in group:
                            piece(*x)

            @pl.when(t + 1 < n)
            def _():
                flip_block(t + 1)

            return carry

        lax.fori_loop(0, hops, sub_epoch, 0)
        for s in range(0, users, 128):
            u_out[pl.ds(s, 128), :] = ut_f[:, pl.ds(s, 128)].T
        for i in range(PIECES):
            hop_copy(hops - 1, i).wait_recv()
        v_out[...] = v_slot[hops]
        for t in range(hops):
            for i in range(PIECES):
                hop_copy(t, i).wait_send()

    return kernel


def flush(u_vmem, v_vmem, u_out, v_out, sem):
    copies = [pltpu.make_async_copy(u_vmem, u_out, sem.at[0]), pltpu.make_async_copy(v_vmem, v_out, sem.at[1])]
    for copy in copies:
        copy.start()
    for copy in copies:
        copy.wait()


def solution(mesh):
    n = mesh.shape["shard"]
    row_spec = P(("rep", "shard"), None)
    hops = EPOCHS * n

    def local_run(ratings, obs_mask, step_counts, user_init, item_init):
        users, rank = user_init.shape
        items = item_init.shape[0]
        f32, bf16 = jnp.float32, jnp.bfloat16
        dma = pltpu.SemaphoreType.DMA
        hbm = pl.BlockSpec(memory_space=pl.ANY)
        vmem = pl.BlockSpec(memory_space=pltpu.VMEM)
        factors = pl.pallas_call(
            make_kernel(n, users, items, rank),
            out_shape=(pltpu.VMEM((users, rank), f32), pltpu.VMEM((items, rank), f32)),
            in_specs=[hbm, hbm, hbm, hbm, hbm],
            out_specs=(vmem, vmem),
            scratch_shapes=[
                pltpu.SMEM((1, n), jnp.int32),
                pltpu.VMEM((n, users, items), f32),
                pltpu.VMEM((n, users, items), jnp.int32),
                pltpu.VMEM((n, items, users), f32),
                pltpu.VMEM((n, items, users), bf16),
                pltpu.VMEM((rank, users), f32),
                pltpu.VMEM((rank, users), bf16),
                pltpu.VMEM((hops + 1, items, rank), f32),
                pltpu.VMEM((hops, items, rank), f32),
                pltpu.VMEM((items, rank), f32),
                pltpu.VMEM((items, users), bf16),
                pltpu.VMEM((rank, items), bf16),
                dma((n,)), dma((n,)), dma, dma, dma, dma((PIECES, hops)), dma((PIECES, hops)),
            ],
            compiler_params=pltpu.CompilerParams(collective_id=0, has_side_effects=True),
            name="dsgd",
        )(step_counts, ratings, obs_mask, user_init, item_init)
        return pl.pallas_call(
            flush,
            out_shape=(jax.ShapeDtypeStruct((users, rank), f32), jax.ShapeDtypeStruct((items, rank), f32)),
            in_specs=[vmem, vmem],
            out_specs=(hbm, hbm),
            scratch_shapes=[dma((2,))],
            compiler_params=pltpu.CompilerParams(vmem_limit_bytes=1 << 20),
            name="flush",
        )(*(pltpu.with_memory_space_constraint(x, pltpu.VMEM) for x in factors))

    return jax.shard_map(local_run, mesh=mesh, in_specs=(row_spec,) * 5, out_specs=(row_spec, row_spec), check_vma=False)
```

```python
import math
import jax
import jax.numpy as jnp
from jax import lax
from jax.experimental import pallas as pl
from jax.experimental.pallas import tpu as pltpu
from jax.sharding import PartitionSpec as P

EPOCHS = 2
STEPS_MAX = 4
TILE = 256


def make_kernel(n, users, items, rank):
    step_size = 0.4 * math.sqrt(rank) / (users + rank)
    decay = 0.1 * items / math.sqrt(rank)
    keep = 1.0 - step_size * decay
    hops = EPOCHS * n
    bf16, f32 = jnp.bfloat16, jnp.float32
    tiles = [(s, min(TILE, users - s)) for s in range(0, users, TILE)]

    def nn(a, b):
        return lax.dot_general(a, b, (((1,), (0,)), ((), ())), preferred_element_type=f32)

    def nt(a, b):
        return lax.dot_general(a, b, (((1,), (1,)), ((), ())), preferred_element_type=f32)

    def split(w, rows):
        return [(0, rows)] if w == TILE else [(0, rows // 2), (rows // 2, rows // 2)]

    def kernel(cnt_hbm, r_hbm, m_hbm, u_hbm, v_hbm, u_out, v_out,
               cnt, r_buf, m_buf, r_t, m_t, ut_f, ut_b, v_slot, v_send, v_f, e_b, vt_b,
               blk_sem, u_sem, v_sem, cnt_sem, recv_sem, send_sem):
        me = lax.axis_index("shard")
        left, right = lax.rem(me + n - 1, n), lax.rem(me + 1, n)

        barrier = pltpu.get_barrier_semaphore()
        for peer in (left, right):
            pl.semaphore_signal(barrier, inc=1, device_id={"shard": peer}, device_id_type=pl.DeviceIdType.MESH)

        def block_copy(kind, q):
            src, dst = ((r_hbm, r_buf), (m_hbm, m_buf))[kind]
            col = pl.multiple_of(lax.rem(me + q, n) * items, items)
            return pltpu.make_async_copy(src.at[:, pl.ds(col, items)], dst.at[q], blk_sem.at[kind, min(q, 1)])

        def block_wait(first, count):
            for kind, buf in enumerate((r_buf, m_buf)):
                blocks = buf.at[pl.ds(first, count)]
                pltpu.make_async_copy(blocks, blocks, blk_sem.at[kind, min(first, 1)]).wait()

        u_in = pltpu.make_async_copy(u_hbm, u_out, u_sem)
        v_in = pltpu.make_async_copy(v_hbm, v_slot.at[0], v_sem)
        cnt_in = pltpu.make_async_copy(cnt_hbm, cnt, cnt_sem)
        block_copy(0, 0).start()
        block_copy(1, 0).start()
        u_in.start()
        v_in.start()
        cnt_in.start()

        def flip_block(q):
            for s in range(0, users, 128):
                rows, cols = pl.ds(s, 128), pl.ds(s, 128)
                marked = jnp.where(m_buf[q, rows, :] != 0, r_buf[q, rows, :], jnp.nan).T
                r_t[q, :, cols] = marked
                m_t[q, :, cols] = jnp.where(marked == marked, 1.0, 0.0).astype(bf16)

        block_wait(0, 1)
        flip_block(0)
        u_in.wait()
        for s in range(0, users, 128):
            flipped = u_out[pl.ds(s, 128), :].T
            ut_f[:, pl.ds(s, 128)] = flipped
            ut_b[:, pl.ds(s, 128)] = flipped.astype(bf16)
        for q in range(1, n):
            block_copy(0, q).start()
            block_copy(1, q).start()
        v_in.wait()
        cnt_in.wait()
        pl.semaphore_wait(barrier, 2)

        def hop_copy(t, last=False):
            return pltpu.make_async_remote_copy(
                src_ref=v_send.at[lax.rem(t, 2)], dst_ref=v_out if last else v_slot.at[t + 1],
                send_sem=send_sem.at[lax.rem(t, 2)], recv_sem=recv_sem.at[lax.rem(t, n)],
                device_id={"shard": left}, device_id_type=pl.DeviceIdType.MESH)

        def sub_epoch(t, carry):
            q = lax.rem(t, n)
            count = cnt[0, lax.rem(me + t, n)]

            @pl.when(t > 0)
            def _():
                hop_copy(t - 1).wait_recv()

            for k in range(STEPS_MAX):
                v_old = (v_slot.at[t] if k == 0 else v_f)[...]
                v_half = v_old.astype(bf16)
                if k == 0:
                    limit, keep_k = 0.5, keep
                    vt_b[...] = v_half.T
                else:
                    live = count > k
                    limit = jnp.where(live, 0.5, 2.0)
                    keep_k = jnp.where(live, keep, 1.0)
                    v_live = jnp.where(jnp.full(v_half.shape, count, jnp.int32) > k, v_old, 0.0).astype(bf16)
                    vt_b[...] = v_live.T

                def pick(new, old):
                    if k == 0:
                        return new
                    return jnp.where(jnp.full(new.shape, count, jnp.int32) > k, new, old)

                for s, w in tiles:
                    cols = pl.ds(s, w)
                    for a, h in split(w, items):
                        approx = nn(v_half[a:a + h], ut_b[:, cols])
                        err = (approx - r_t[q, pl.ds(a, h), cols]).astype(bf16)
                        seen = m_t[q, pl.ds(a, h), cols] > jnp.full((h, w), limit, f32).astype(bf16)
                        e_b[pl.ds(a, h), cols] = jnp.where(seen, err, jnp.zeros_like(err))
                half = items // 2
                parts = [keep * v_old[i * half:(i + 1) * half] for i in range(2)]

                def item_grad(s, w):
                    cols = pl.ds(s, w)
                    if w == TILE:
                        g = step_size * nt(e_b[:, cols], ut_b[:, cols])
                        for i in range(2):
                            parts[i] = parts[i] - g[i * half:(i + 1) * half]
                    else:
                        for i in range(2):
                            parts[i] = parts[i] - step_size * nt(e_b[pl.ds(i * half, half), cols], ut_b[:, cols])

                def item_update():
                    v_new = pick(jnp.concatenate(parts, axis=0), v_old)
                    if k < STEPS_MAX - 1:
                        v_f[...] = v_new
                    else:
                        v_send[lax.rem(t, 2)] = v_new

                        @pl.when(t < hops - 1)
                        def _():
                            hop_copy(t).start()

                        @pl.when(t == hops - 1)
                        def _():
                            hop_copy(t, last=True).start()

                def user_update(s, w):
                    cols = pl.ds(s, w)
                    for a, h in split(w, rank):
                        rows = pl.ds(a, h)
                        grad = nn(vt_b[rows, :], e_b[:, cols])
                        u_new = keep_k * ut_f[rows, cols] - step_size * grad
                        ut_f[rows, cols] = u_new
                        ut_b[rows, cols] = u_new.astype(bf16)

                wide = [x for x in tiles if x[1] == TILE]
                narrow = [x for x in tiles if x[1] < TILE]
                if k < STEPS_MAX - 1:
                    order = [(item_grad, wide), (user_update, wide), (item_grad, narrow), (item_update, None), (user_update, narrow)]
                else:
                    order = [(item_grad, wide), (item_grad, narrow), (item_update, None), (user_update, wide), (user_update, narrow)]
                for piece, group in order:
                    if group is None:
                        piece()
                    else:
                        for x in group:
                            piece(*x)

            @pl.when(t == 0)
            def _():
                block_wait(1, n - 1)

            @pl.when(t + 1 < n)
            def _():
                flip_block(t + 1)

            @pl.when(t > 0)
            def _():
                hop_copy(t - 1).wait_send()

            return carry

        lax.fori_loop(0, hops, sub_epoch, 0)
        for s in range(0, users, 128):
            u_out[pl.ds(s, 128), :] = ut_f[:, pl.ds(s, 128)].T
        hop_copy(hops - 1, last=True).wait_recv()
        hop_copy(hops - 1, last=True).wait_send()

    return kernel


def flush(u_vmem, v_vmem, u_out, v_out, sem):
    copies = [pltpu.make_async_copy(u_vmem, u_out, sem.at[0]), pltpu.make_async_copy(v_vmem, v_out, sem.at[1])]
    for copy in copies:
        copy.start()
    for copy in copies:
        copy.wait()


def solution(mesh):
    n = mesh.shape["shard"]
    row_spec = P(("rep", "shard"), None)
    hops = EPOCHS * n

    def local_run(ratings, obs_mask, step_counts, user_init, item_init):
        users, rank = user_init.shape
        items = item_init.shape[0]
        f32, bf16 = jnp.float32, jnp.bfloat16
        dma = pltpu.SemaphoreType.DMA
        hbm = pl.BlockSpec(memory_space=pl.ANY)
        vmem = pl.BlockSpec(memory_space=pltpu.VMEM)
        factors = pl.pallas_call(
            make_kernel(n, users, items, rank),
            out_shape=(pltpu.VMEM((users, rank), f32), pltpu.VMEM((items, rank), f32)),
            in_specs=[hbm, hbm, hbm, hbm, hbm],
            out_specs=(vmem, vmem),
            scratch_shapes=[
                pltpu.SMEM((1, n), jnp.int32),
                pltpu.VMEM((n, users, items), f32),
                pltpu.VMEM((n, users, items), jnp.int32),
                pltpu.VMEM((n, items, users), f32),
                pltpu.VMEM((n, items, users), bf16),
                pltpu.VMEM((rank, users), f32),
                pltpu.VMEM((rank, users), bf16),
                pltpu.VMEM((hops, items, rank), f32),
                pltpu.VMEM((2, items, rank), f32),
                pltpu.VMEM((items, rank), f32),
                pltpu.VMEM((items, users), bf16),
                pltpu.VMEM((rank, items), bf16),
                dma((2, 2)), dma, dma, dma, dma((n,)), dma((2,)),
            ],
            compiler_params=pltpu.CompilerParams(collective_id=0, has_side_effects=True),
            name="dsgd",
        )(step_counts, ratings, obs_mask, user_init, item_init)
        return pl.pallas_call(
            flush,
            out_shape=(jax.ShapeDtypeStruct((users, rank), f32), jax.ShapeDtypeStruct((items, rank), f32)),
            in_specs=[vmem, vmem],
            out_specs=(hbm, hbm),
            scratch_shapes=[dma((2,))],
            compiler_params=pltpu.CompilerParams(vmem_limit_bytes=1 << 20),
            name="flush",
        )(*(pltpu.with_memory_space_constraint(x, pltpu.VMEM) for x in factors))

    return jax.shard_map(local_run, mesh=mesh, in_specs=(row_spec,) * 5, out_specs=(row_spec, row_spec), check_vma=False)
```

```python
import math
import jax
import jax.numpy as jnp
from jax import lax
from jax.experimental import pallas as pl
from jax.experimental.pallas import tpu as pltpu
from jax.sharding import PartitionSpec as P

EPOCHS = 2
STEPS_MAX = 4
TILE = 256


def make_kernel(n, users, items, rank):
    step_size = 0.4 * math.sqrt(rank) / (users + rank)
    decay = 0.1 * items / math.sqrt(rank)
    keep = 1.0 - step_size * decay
    hops = EPOCHS * n
    bf16, f32 = jnp.bfloat16, jnp.float32
    tiles = [(s, min(TILE, users - s)) for s in range(0, users, TILE)]

    def nn(a, b):
        return lax.dot_general(a, b, (((1,), (0,)), ((), ())), preferred_element_type=f32)

    def nt(a, b):
        return lax.dot_general(a, b, (((1,), (1,)), ((), ())), preferred_element_type=f32)

    def split(w, rows):
        return [(0, rows)] if w == TILE else [(0, rows // 2), (rows // 2, rows // 2)]

    def kernel(cnt_hbm, r_hbm, m_hbm, u_hbm, v_hbm, u_out, v_out,
               cnt, r_buf, m_buf, r_t, m_t, ut_f, ut_b, v_slot, v_send, v_f, e_b, vt_b,
               blk_sem, u_sem, v_sem, cnt_sem, recv_sem, send_sem):
        me = lax.axis_index("shard")
        left, right = lax.rem(me + n - 1, n), lax.rem(me + 1, n)

        barrier = pltpu.get_barrier_semaphore()
        for peer in (left, right):
            pl.semaphore_signal(barrier, inc=1, device_id={"shard": peer}, device_id_type=pl.DeviceIdType.MESH)

        def block_copy(kind, q):
            src, dst = ((r_hbm, r_buf), (m_hbm, m_buf))[kind]
            col = pl.multiple_of(lax.rem(me + q, n) * items, items)
            return pltpu.make_async_copy(src.at[:, pl.ds(col, items)], dst.at[q], blk_sem.at[kind, min(q, 1)])

        def block_wait(first, count):
            for kind, buf in enumerate((r_buf, m_buf)):
                blocks = buf.at[pl.ds(first, count)]
                pltpu.make_async_copy(blocks, blocks, blk_sem.at[kind, min(first, 1)]).wait()

        u_in = pltpu.make_async_copy(u_hbm, u_out, u_sem)
        v_in = pltpu.make_async_copy(v_hbm, v_slot.at[0], v_sem)
        cnt_in = pltpu.make_async_copy(cnt_hbm, cnt, cnt_sem)
        u_in.start()
        block_copy(0, 0).start()
        block_copy(1, 0).start()
        v_in.start()
        cnt_in.start()

        def flip_block(q):
            for s in range(0, users, 128):
                rows, cols = pl.ds(s, 128), pl.ds(s, 128)
                marked = jnp.where(m_buf[q, rows, :] != 0, r_buf[q, rows, :], jnp.nan).T
                r_t[q, :, cols] = marked
                m_t[q, :, cols] = jnp.where(marked == marked, 1.0, 0.0).astype(bf16)

        u_in.wait()
        for s in range(0, users, 128):
            flipped = u_out[pl.ds(s, 128), :].T
            ut_f[:, pl.ds(s, 128)] = flipped
            ut_b[:, pl.ds(s, 128)] = flipped.astype(bf16)
        block_wait(0, 1)
        for q in range(1, n):
            block_copy(0, q).start()
            block_copy(1, q).start()
        flip_block(0)
        v_in.wait()
        cnt_in.wait()
        pl.semaphore_wait(barrier, 2)

        def hop_copy(t, last=False):
            return pltpu.make_async_remote_copy(
                src_ref=v_send.at[lax.rem(t, 2)], dst_ref=v_out if last else v_slot.at[t + 1],
                send_sem=send_sem.at[lax.rem(t, 2)], recv_sem=recv_sem.at[lax.rem(t, n)],
                device_id={"shard": left}, device_id_type=pl.DeviceIdType.MESH)

        def sub_epoch(t, carry):
            q = lax.rem(t, n)
            count = cnt[0, lax.rem(me + t, n)]

            @pl.when(t > 0)
            def _():
                hop_copy(t - 1).wait_recv()

            for k in range(STEPS_MAX):
                v_old = (v_slot.at[t] if k == 0 else v_f)[...]
                v_half = v_old.astype(bf16)
                if k == 0:
                    limit, keep_k = 0.5, keep
                    vt_b[...] = v_half.T
                else:
                    live = count > k
                    limit = jnp.where(live, 0.5, 2.0)
                    keep_k = jnp.where(live, keep, 1.0)
                    v_live = jnp.where(jnp.full(v_half.shape, count, jnp.int32) > k, v_old, 0.0).astype(bf16)
                    vt_b[...] = v_live.T

                def pick(new, old):
                    if k == 0:
                        return new
                    return jnp.where(jnp.full(new.shape, count, jnp.int32) > k, new, old)

                for s, w in tiles:
                    cols = pl.ds(s, w)
                    for a, h in split(w, items):
                        approx = nn(v_half[a:a + h], ut_b[:, cols])
                        err = (approx - r_t[q, pl.ds(a, h), cols]).astype(bf16)
                        seen = m_t[q, pl.ds(a, h), cols] > jnp.full((h, w), limit, f32).astype(bf16)
                        e_b[pl.ds(a, h), cols] = jnp.where(seen, err, jnp.zeros_like(err))
                half = items // 2
                parts = [keep * v_old[i * half:(i + 1) * half] for i in range(2)]

                def item_grad(s, w):
                    cols = pl.ds(s, w)
                    if w == TILE:
                        g = step_size * nt(e_b[:, cols], ut_b[:, cols])
                        for i in range(2):
                            parts[i] = parts[i] - g[i * half:(i + 1) * half]
                    else:
                        for i in range(2):
                            parts[i] = parts[i] - step_size * nt(e_b[pl.ds(i * half, half), cols], ut_b[:, cols])

                def item_update():
                    v_new = pick(jnp.concatenate(parts, axis=0), v_old)
                    if k < STEPS_MAX - 1:
                        v_f[...] = v_new
                    else:
                        v_send[lax.rem(t, 2)] = v_new

                        @pl.when(t < hops - 1)
                        def _():
                            hop_copy(t).start()

                        @pl.when(t == hops - 1)
                        def _():
                            hop_copy(t, last=True).start()

                def user_update(s, w):
                    cols = pl.ds(s, w)
                    for a, h in split(w, rank):
                        rows = pl.ds(a, h)
                        grad = nn(vt_b[rows, :], e_b[:, cols])
                        u_new = keep_k * ut_f[rows, cols] - step_size * grad
                        ut_f[rows, cols] = u_new
                        ut_b[rows, cols] = u_new.astype(bf16)

                wide = [x for x in tiles if x[1] == TILE]
                narrow = [x for x in tiles if x[1] < TILE]
                if k < STEPS_MAX - 1:
                    order = [(item_grad, wide), (user_update, wide), (item_grad, narrow), (item_update, None), (user_update, narrow)]
                else:
                    order = [(item_grad, wide), (item_grad, narrow), (item_update, None), (user_update, wide), (user_update, narrow)]
                for piece, group in order:
                    if group is None:
                        piece()
                    else:
                        for x in group:
                            piece(*x)

            @pl.when(t == 0)
            def _():
                block_wait(1, n - 1)

            @pl.when(t + 1 < n)
            def _():
                flip_block(t + 1)

            @pl.when(t > 0)
            def _():
                hop_copy(t - 1).wait_send()

            return carry

        lax.fori_loop(0, hops, sub_epoch, 0)
        for s in range(0, users, 128):
            u_out[pl.ds(s, 128), :] = ut_f[:, pl.ds(s, 128)].T
        hop_copy(hops - 1, last=True).wait_recv()
        hop_copy(hops - 1, last=True).wait_send()

    return kernel


def flush(u_vmem, v_vmem, u_out, v_out, sem):
    copies = [pltpu.make_async_copy(u_vmem, u_out, sem.at[0]), pltpu.make_async_copy(v_vmem, v_out, sem.at[1])]
    for copy in copies:
        copy.start()
    for copy in copies:
        copy.wait()


def solution(mesh):
    n = mesh.shape["shard"]
    row_spec = P(("rep", "shard"), None)
    hops = EPOCHS * n

    def local_run(ratings, obs_mask, step_counts, user_init, item_init):
        users, rank = user_init.shape
        items = item_init.shape[0]
        f32, bf16 = jnp.float32, jnp.bfloat16
        dma = pltpu.SemaphoreType.DMA
        hbm = pl.BlockSpec(memory_space=pl.ANY)
        vmem = pl.BlockSpec(memory_space=pltpu.VMEM)
        factors = pl.pallas_call(
            make_kernel(n, users, items, rank),
            out_shape=(pltpu.VMEM((users, rank), f32), pltpu.VMEM((items, rank), f32)),
            in_specs=[hbm, hbm, hbm, hbm, hbm],
            out_specs=(vmem, vmem),
            scratch_shapes=[
                pltpu.SMEM((1, n), jnp.int32),
                pltpu.VMEM((n, users, items), f32),
                pltpu.VMEM((n, users, items), jnp.int32),
                pltpu.VMEM((n, items, users), f32),
                pltpu.VMEM((n, items, users), bf16),
                pltpu.VMEM((rank, users), f32),
                pltpu.VMEM((rank, users), bf16),
                pltpu.VMEM((hops, items, rank), f32),
                pltpu.VMEM((2, items, rank), f32),
                pltpu.VMEM((items, rank), f32),
                pltpu.VMEM((items, users), bf16),
                pltpu.VMEM((rank, items), bf16),
                dma((2, 2)), dma, dma, dma, dma((n,)), dma((2,)),
            ],
            compiler_params=pltpu.CompilerParams(collective_id=0, has_side_effects=True),
            name="dsgd",
        )(step_counts, ratings, obs_mask, user_init, item_init)
        return pl.pallas_call(
            flush,
            out_shape=(jax.ShapeDtypeStruct((users, rank), f32), jax.ShapeDtypeStruct((items, rank), f32)),
            in_specs=[vmem, vmem],
            out_specs=(hbm, hbm),
            scratch_shapes=[dma((2,))],
            compiler_params=pltpu.CompilerParams(vmem_limit_bytes=1 << 20),
            name="flush",
        )(*(pltpu.with_memory_space_constraint(x, pltpu.VMEM) for x in factors))

    return jax.shard_map(local_run, mesh=mesh, in_specs=(row_spec,) * 5, out_specs=(row_spec, row_spec), check_vma=False)
```

```python
import math
import jax
import jax.numpy as jnp
from jax import lax
from jax.experimental import pallas as pl
from jax.experimental.pallas import tpu as pltpu
from jax.sharding import PartitionSpec as P

EPOCHS = 2
STEPS_MAX = 4
TILE = 256


def make_kernel(n, users, items, rank):
    step_size = 0.4 * math.sqrt(rank) / (users + rank)
    decay = 0.1 * items / math.sqrt(rank)
    keep = 1.0 - step_size * decay
    hops = EPOCHS * n
    bf16, f32 = jnp.bfloat16, jnp.float32
    tiles = [(s, min(TILE, users - s)) for s in range(0, users, TILE)]

    def nn(a, b):
        return lax.dot_general(a, b, (((1,), (0,)), ((), ())), preferred_element_type=f32)

    def nt(a, b):
        return lax.dot_general(a, b, (((1,), (1,)), ((), ())), preferred_element_type=f32)

    def split(w, rows):
        return [(0, rows)] if w == TILE else [(0, rows // 2), (rows // 2, rows // 2)]

    def kernel(cnt_hbm, r_hbm, m_hbm, u_hbm, v_hbm, u_out, v_out,
               cnt, r_buf, m_buf, r_t, m_t, ut_f, ut_b, u_b, v_slot, v_send, v_f, e_b, vt_b,
               blk_sem, u_sem, v_sem, cnt_sem, recv_sem, send_sem):
        me = lax.axis_index("shard")
        left, right = lax.rem(me + n - 1, n), lax.rem(me + 1, n)

        barrier = pltpu.get_barrier_semaphore()
        for peer in (left, right):
            pl.semaphore_signal(barrier, inc=1, device_id={"shard": peer}, device_id_type=pl.DeviceIdType.MESH)

        def block_copy(kind, q):
            src, dst = ((r_hbm, r_buf), (m_hbm, m_buf))[kind]
            col = pl.multiple_of(lax.rem(me + q, n) * items, items)
            return pltpu.make_async_copy(src.at[:, pl.ds(col, items)], dst.at[q], blk_sem.at[kind, min(q, 1)])

        def block_wait(first, count):
            for kind, buf in enumerate((r_buf, m_buf)):
                blocks = buf.at[pl.ds(first, count)]
                pltpu.make_async_copy(blocks, blocks, blk_sem.at[kind, min(first, 1)]).wait()

        u_in = pltpu.make_async_copy(u_hbm, u_out, u_sem)
        v_in = pltpu.make_async_copy(v_hbm, v_slot.at[0], v_sem)
        cnt_in = pltpu.make_async_copy(cnt_hbm, cnt, cnt_sem)
        u_in.start()
        block_copy(0, 0).start()
        block_copy(1, 0).start()
        v_in.start()
        cnt_in.start()

        def flip_block(q):
            for s in range(0, users, 128):
                rows, cols = pl.ds(s, 128), pl.ds(s, 128)
                marked = jnp.where(m_buf[q, rows, :] != 0, r_buf[q, rows, :], jnp.nan).T
                r_t[q, :, cols] = marked
                m_t[q, :, cols] = jnp.where(marked == marked, 1.0, 0.0).astype(bf16)

        u_in.wait()
        for s in range(0, users, 128):
            flipped = u_out[pl.ds(s, 128), :].T
            ut_f[:, pl.ds(s, 128)] = flipped
            ut_b[:, pl.ds(s, 128)] = flipped.astype(bf16)
            u_b[pl.ds(s, 128), :] = u_out[pl.ds(s, 128), :].astype(bf16)
        block_wait(0, 1)
        for q in range(1, n):
            block_copy(0, q).start()
            block_copy(1, q).start()
        flip_block(0)
        v_in.wait()
        cnt_in.wait()
        pl.semaphore_wait(barrier, 2)

        def hop_copy(t, last=False):
            return pltpu.make_async_remote_copy(
                src_ref=v_send.at[lax.rem(t, 2)], dst_ref=v_out if last else v_slot.at[t + 1],
                send_sem=send_sem.at[lax.rem(t, 2)], recv_sem=recv_sem.at[lax.rem(t, n)],
                device_id={"shard": left}, device_id_type=pl.DeviceIdType.MESH)

        def sub_epoch(t, carry):
            q = lax.rem(t, n)
            count = cnt[0, lax.rem(me + t, n)]

            @pl.when(t > 0)
            def _():
                hop_copy(t - 1).wait_recv()

            for k in range(STEPS_MAX):
                v_old = (v_slot.at[t] if k == 0 else v_f)[...]
                v_half = v_old.astype(bf16)
                if k == 0:
                    limit, keep_k = 0.5, keep
                    vt_b[...] = v_half.T
                else:
                    live = count > k
                    limit = jnp.where(live, 0.5, 2.0)
                    keep_k = jnp.where(live, keep, 1.0)
                    v_live = jnp.where(jnp.full(v_half.shape, count, jnp.int32) > k, v_old, 0.0).astype(bf16)
                    vt_b[...] = v_live.T

                def pick(new, old):
                    if k == 0:
                        return new
                    return jnp.where(jnp.full(new.shape, count, jnp.int32) > k, new, old)

                for s, w in tiles:
                    cols = pl.ds(s, w)
                    for a, h in split(w, items):
                        approx = nn(v_half[a:a + h], ut_b[:, cols])
                        err = (approx - r_t[q, pl.ds(a, h), cols]).astype(bf16)
                        seen = m_t[q, pl.ds(a, h), cols] > jnp.full((h, w), limit, f32).astype(bf16)
                        e_b[pl.ds(a, h), cols] = jnp.where(seen, err, jnp.zeros_like(err))
                half = items // 2
                parts = [keep * v_old[i * half:(i + 1) * half] for i in range(2)]

                def item_grad(s, w):
                    cols = pl.ds(s, w)
                    if w == TILE:
                        g = step_size * nn(e_b[:, cols], u_b[cols, :])
                        for i in range(2):
                            parts[i] = parts[i] - g[i * half:(i + 1) * half]
                    else:
                        for i in range(2):
                            parts[i] = parts[i] - step_size * nn(e_b[pl.ds(i * half, half), cols], u_b[cols, :])

                def item_update():
                    v_new = pick(jnp.concatenate(parts, axis=0), v_old)
                    if k < STEPS_MAX - 1:
                        v_f[...] = v_new
                    else:
                        v_send[lax.rem(t, 2)] = v_new

                        @pl.when(t < hops - 1)
                        def _():
                            hop_copy(t).start()

                        @pl.when(t == hops - 1)
                        def _():
                            hop_copy(t, last=True).start()

                def user_update(s, w):
                    cols = pl.ds(s, w)
                    for a, h in split(w, rank):
                        rows = pl.ds(a, h)
                        grad = nn(vt_b[rows, :], e_b[:, cols])
                        u_new = keep_k * ut_f[rows, cols] - step_size * grad
                        ut_f[rows, cols] = u_new
                        u_half = u_new.astype(bf16)
                        ut_b[rows, cols] = u_half
                        u_b[cols, rows] = u_half.T

                wide = [x for x in tiles if x[1] == TILE]
                narrow = [x for x in tiles if x[1] < TILE]
                if k < STEPS_MAX - 1:
                    order = [(item_grad, wide), (user_update, wide), (item_grad, narrow), (item_update, None), (user_update, narrow)]
                else:
                    order = [(item_grad, wide), (item_grad, narrow), (item_update, None), (user_update, wide), (user_update, narrow)]
                for piece, group in order:
                    if group is None:
                        piece()
                    else:
                        for x in group:
                            piece(*x)

            @pl.when(t == 0)
            def _():
                block_wait(1, n - 1)

            @pl.when(t + 1 < n)
            def _():
                flip_block(t + 1)

            @pl.when(t > 0)
            def _():
                hop_copy(t - 1).wait_send()

            return carry

        lax.fori_loop(0, hops, sub_epoch, 0)
        for s in range(0, users, 128):
            u_out[pl.ds(s, 128), :] = ut_f[:, pl.ds(s, 128)].T
        hop_copy(hops - 1, last=True).wait_recv()
        hop_copy(hops - 1, last=True).wait_send()

    return kernel


def flush(u_vmem, v_vmem, u_out, v_out, sem):
    copies = [pltpu.make_async_copy(u_vmem, u_out, sem.at[0]), pltpu.make_async_copy(v_vmem, v_out, sem.at[1])]
    for copy in copies:
        copy.start()
    for copy in copies:
        copy.wait()


def solution(mesh):
    n = mesh.shape["shard"]
    row_spec = P(("rep", "shard"), None)
    hops = EPOCHS * n

    def local_run(ratings, obs_mask, step_counts, user_init, item_init):
        users, rank = user_init.shape
        items = item_init.shape[0]
        f32, bf16 = jnp.float32, jnp.bfloat16
        dma = pltpu.SemaphoreType.DMA
        hbm = pl.BlockSpec(memory_space=pl.ANY)
        vmem = pl.BlockSpec(memory_space=pltpu.VMEM)
        factors = pl.pallas_call(
            make_kernel(n, users, items, rank),
            out_shape=(pltpu.VMEM((users, rank), f32), pltpu.VMEM((items, rank), f32)),
            in_specs=[hbm, hbm, hbm, hbm, hbm],
            out_specs=(vmem, vmem),
            scratch_shapes=[
                pltpu.SMEM((1, n), jnp.int32),
                pltpu.VMEM((n, users, items), f32),
                pltpu.VMEM((n, users, items), jnp.int32),
                pltpu.VMEM((n, items, users), f32),
                pltpu.VMEM((n, items, users), bf16),
                pltpu.VMEM((rank, users), f32),
                pltpu.VMEM((rank, users), bf16),
                pltpu.VMEM((users, rank), bf16),
                pltpu.VMEM((hops, items, rank), f32),
                pltpu.VMEM((2, items, rank), f32),
                pltpu.VMEM((items, rank), f32),
                pltpu.VMEM((items, users), bf16),
                pltpu.VMEM((rank, items), bf16),
                dma((2, 2)), dma, dma, dma, dma((n,)), dma((2,)),
            ],
            compiler_params=pltpu.CompilerParams(collective_id=0, has_side_effects=True),
            name="dsgd",
        )(step_counts, ratings, obs_mask, user_init, item_init)
        return pl.pallas_call(
            flush,
            out_shape=(jax.ShapeDtypeStruct((users, rank), f32), jax.ShapeDtypeStruct((items, rank), f32)),
            in_specs=[vmem, vmem],
            out_specs=(hbm, hbm),
            scratch_shapes=[dma((2,))],
            compiler_params=pltpu.CompilerParams(vmem_limit_bytes=1 << 20),
            name="flush",
        )(*(pltpu.with_memory_space_constraint(x, pltpu.VMEM) for x in factors))

    return jax.shard_map(local_run, mesh=mesh, in_specs=(row_spec,) * 5, out_specs=(row_spec, row_spec), check_vma=False)
```

```python
import math
import jax
import jax.numpy as jnp
from jax import lax
from jax.experimental import pallas as pl
from jax.experimental.pallas import tpu as pltpu
from jax.sharding import PartitionSpec as P

EPOCHS = 2
STEPS_MAX = 4
TILE = 256
PIECE = 128


def make_kernel(n, users, items, rank):
    step_size = 0.4 * math.sqrt(rank) / (users + rank)
    decay = 0.1 * items / math.sqrt(rank)
    keep = 1.0 - step_size * decay
    hops = EPOCHS * n
    bf16, f32 = jnp.bfloat16, jnp.float32
    tiles = [(s, min(TILE, users - s)) for s in range(0, users, TILE)]

    def nn(a, b):
        return lax.dot_general(a, b, (((1,), (0,)), ((), ())), preferred_element_type=f32)

    def nt(a, b):
        return lax.dot_general(a, b, (((1,), (1,)), ((), ())), preferred_element_type=f32)

    def split(w, rows):
        return [(0, rows)] if w == TILE else [(0, rows // 2), (rows // 2, rows // 2)]

    def kernel(cnt_hbm, r_hbm, m_hbm, u_hbm, v_hbm, u_out, v_out,
               cnt, r_buf, m_buf, r_t, m_t, ut_f, ut_b, v_slot, v_send, v_f, e_b, vt_b,
               blk_sem, u_sem, v_sem, cnt_sem, recv_sem, send_sem):
        me = lax.axis_index("shard")
        left, right = lax.rem(me + n - 1, n), lax.rem(me + 1, n)

        barrier = pltpu.get_barrier_semaphore()
        for peer in (left, right):
            pl.semaphore_signal(barrier, inc=1, device_id={"shard": peer}, device_id_type=pl.DeviceIdType.MESH)

        def fetch_block(q):
            col = pl.multiple_of(lax.rem(me + q, n) * items, items)
            for s in range(0, users, PIECE):
                for kind, (src, dst) in enumerate(((r_hbm, r_buf), (m_hbm, m_buf))):
                    pltpu.make_async_copy(src.at[pl.ds(s, PIECE), pl.ds(col, items)], dst.at[q, pl.ds(s, PIECE)],
                                          blk_sem.at[kind, min(q, 1)]).start()

        def block_wait(first, count):
            for kind, buf in enumerate((r_buf, m_buf)):
                blocks = buf.at[pl.ds(first, count)]
                pltpu.make_async_copy(blocks, blocks, blk_sem.at[kind, min(first, 1)]).wait()

        u_in = pltpu.make_async_copy(u_hbm, u_out, u_sem)
        v_in = pltpu.make_async_copy(v_hbm, v_slot.at[0], v_sem)
        cnt_in = pltpu.make_async_copy(cnt_hbm, cnt, cnt_sem)
        for s in range(0, users, PIECE):
            pltpu.make_async_copy(u_hbm.at[pl.ds(s, PIECE)], u_out.at[pl.ds(s, PIECE)], u_sem).start()
        fetch_block(0)
        v_in.start()
        cnt_in.start()

        def flip_block(q):
            for s in range(0, users, 128):
                rows, cols = pl.ds(s, 128), pl.ds(s, 128)
                marked = jnp.where(m_buf[q, rows, :] != 0, r_buf[q, rows, :], jnp.nan).T
                r_t[q, :, cols] = marked
                m_t[q, :, cols] = jnp.where(marked == marked, 1.0, 0.0).astype(bf16)

        u_in.wait()
        for s in range(0, users, 128):
            flipped = u_out[pl.ds(s, 128), :].T
            ut_f[:, pl.ds(s, 128)] = flipped
            ut_b[:, pl.ds(s, 128)] = flipped.astype(bf16)
        block_wait(0, 1)
        for q in range(1, n):
            fetch_block(q)
        flip_block(0)
        v_in.wait()
        cnt_in.wait()
        pl.semaphore_wait(barrier, 2)

        def hop_copy(t, last=False):
            return pltpu.make_async_remote_copy(
                src_ref=v_send.at[lax.rem(t, 2)], dst_ref=v_out if last else v_slot.at[t + 1],
                send_sem=send_sem.at[lax.rem(t, 2)], recv_sem=recv_sem.at[lax.rem(t, n)],
                device_id={"shard": left}, device_id_type=pl.DeviceIdType.MESH)

        def sub_epoch(t, carry):
            q = lax.rem(t, n)
            count = cnt[0, lax.rem(me + t, n)]

            @pl.when(t > 0)
            def _():
                hop_copy(t - 1).wait_recv()

            for k in range(STEPS_MAX):
                v_old = (v_slot.at[t] if k == 0 else v_f)[...]
                v_half = v_old.astype(bf16)
                if k == 0:
                    limit, keep_k = 0.5, keep
                    vt_b[...] = v_half.T
                else:
                    live = count > k
                    limit = jnp.where(live, 0.5, 2.0)
                    keep_k = jnp.where(live, keep, 1.0)
                    v_live = jnp.where(jnp.full(v_half.shape, count, jnp.int32) > k, v_old, 0.0).astype(bf16)
                    vt_b[...] = v_live.T

                def pick(new, old):
                    if k == 0:
                        return new
                    return jnp.where(jnp.full(new.shape, count, jnp.int32) > k, new, old)

                for s, w in tiles:
                    cols = pl.ds(s, w)
                    for a, h in split(w, items):
                        approx = nn(v_half[a:a + h], ut_b[:, cols])
                        err = (approx - r_t[q, pl.ds(a, h), cols]).astype(bf16)
                        seen = m_t[q, pl.ds(a, h), cols] > jnp.full((h, w), limit, f32).astype(bf16)
                        e_b[pl.ds(a, h), cols] = jnp.where(seen, err, jnp.zeros_like(err))
                half = items // 2
                parts = [keep * v_old[i * half:(i + 1) * half] for i in range(2)]

                def item_grad(s, w):
                    cols = pl.ds(s, w)
                    if w == TILE:
                        g = step_size * nt(e_b[:, cols], ut_b[:, cols])
                        for i in range(2):
                            parts[i] = parts[i] - g[i * half:(i + 1) * half]
                    else:
                        for i in range(2):
                            parts[i] = parts[i] - step_size * nt(e_b[pl.ds(i * half, half), cols], ut_b[:, cols])

                def item_update():
                    v_new = pick(jnp.concatenate(parts, axis=0), v_old)
                    if k < STEPS_MAX - 1:
                        v_f[...] = v_new
                    else:
                        v_send[lax.rem(t, 2)] = v_new

                        @pl.when(t < hops - 1)
                        def _():
                            hop_copy(t).start()

                        @pl.when(t == hops - 1)
                        def _():
                            hop_copy(t, last=True).start()

                def user_update(s, w):
                    cols = pl.ds(s, w)
                    for a, h in split(w, rank):
                        rows = pl.ds(a, h)
                        grad = nn(vt_b[rows, :], e_b[:, cols])
                        u_new = keep_k * ut_f[rows, cols] - step_size * grad
                        ut_f[rows, cols] = u_new
                        ut_b[rows, cols] = u_new.astype(bf16)

                wide = [x for x in tiles if x[1] == TILE]
                narrow = [x for x in tiles if x[1] < TILE]
                if k < STEPS_MAX - 1:
                    order = [(item_grad, wide), (user_update, wide), (item_grad, narrow), (item_update, None), (user_update, narrow)]
                else:
                    order = [(item_grad, wide), (item_grad, narrow), (item_update, None), (user_update, wide), (user_update, narrow)]
                for piece, group in order:
                    if group is None:
                        piece()
                    else:
                        for x in group:
                            piece(*x)

            @pl.when(t == 0)
            def _():
                block_wait(1, n - 1)

            @pl.when(t + 1 < n)
            def _():
                flip_block(t + 1)

            @pl.when(t > 0)
            def _():
                hop_copy(t - 1).wait_send()

            return carry

        lax.fori_loop(0, hops, sub_epoch, 0)
        for s in range(0, users, 128):
            u_out[pl.ds(s, 128), :] = ut_f[:, pl.ds(s, 128)].T
        hop_copy(hops - 1, last=True).wait_recv()
        hop_copy(hops - 1, last=True).wait_send()

    return kernel


def flush(u_vmem, v_vmem, u_out, v_out, sem):
    v_copy = pltpu.make_async_copy(v_vmem, v_out, sem.at[1])
    v_copy.start()
    for s in range(0, u_vmem.shape[0], PIECE):
        pltpu.make_async_copy(u_vmem.at[pl.ds(s, PIECE)], u_out.at[pl.ds(s, PIECE)], sem.at[0]).start()
    v_copy.wait()
    pltpu.make_async_copy(u_vmem, u_out, sem.at[0]).wait()


def solution(mesh):
    n = mesh.shape["shard"]
    row_spec = P(("rep", "shard"), None)
    hops = EPOCHS * n

    def local_run(ratings, obs_mask, step_counts, user_init, item_init):
        users, rank = user_init.shape
        items = item_init.shape[0]
        f32, bf16 = jnp.float32, jnp.bfloat16
        dma = pltpu.SemaphoreType.DMA
        hbm = pl.BlockSpec(memory_space=pl.ANY)
        vmem = pl.BlockSpec(memory_space=pltpu.VMEM)
        factors = pl.pallas_call(
            make_kernel(n, users, items, rank),
            out_shape=(pltpu.VMEM((users, rank), f32), pltpu.VMEM((items, rank), f32)),
            in_specs=[hbm, hbm, hbm, hbm, hbm],
            out_specs=(vmem, vmem),
            scratch_shapes=[
                pltpu.SMEM((1, n), jnp.int32),
                pltpu.VMEM((n, users, items), f32),
                pltpu.VMEM((n, users, items), jnp.int32),
                pltpu.VMEM((n, items, users), f32),
                pltpu.VMEM((n, items, users), bf16),
                pltpu.VMEM((rank, users), f32),
                pltpu.VMEM((rank, users), bf16),
                pltpu.VMEM((hops, items, rank), f32),
                pltpu.VMEM((2, items, rank), f32),
                pltpu.VMEM((items, rank), f32),
                pltpu.VMEM((items, users), bf16),
                pltpu.VMEM((rank, items), bf16),
                dma((2, 2)), dma, dma, dma, dma((n,)), dma((2,)),
            ],
            compiler_params=pltpu.CompilerParams(collective_id=0, has_side_effects=True),
            name="dsgd",
        )(step_counts, ratings, obs_mask, user_init, item_init)
        return pl.pallas_call(
            flush,
            out_shape=(jax.ShapeDtypeStruct((users, rank), f32), jax.ShapeDtypeStruct((items, rank), f32)),
            in_specs=[vmem, vmem],
            out_specs=(hbm, hbm),
            scratch_shapes=[dma((2,))],
            compiler_params=pltpu.CompilerParams(vmem_limit_bytes=1 << 20),
            name="flush",
        )(*(pltpu.with_memory_space_constraint(x, pltpu.VMEM) for x in factors))

    return jax.shard_map(local_run, mesh=mesh, in_specs=(row_spec,) * 5, out_specs=(row_spec, row_spec), check_vma=False)
```

```python
import math
import jax
import jax.numpy as jnp
from jax import lax
from jax.experimental import pallas as pl
from jax.experimental.pallas import tpu as pltpu
from jax.sharding import PartitionSpec as P

EPOCHS = 2
STEPS_MAX = 4
TILE = 256


def make_kernel(n, users, items, rank):
    step_size = 0.4 * math.sqrt(rank) / (users + rank)
    decay = 0.1 * items / math.sqrt(rank)
    keep = 1.0 - step_size * decay
    hops = EPOCHS * n
    bf16, f32 = jnp.bfloat16, jnp.float32
    tiles = [(s, min(TILE, users - s)) for s in range(0, users, TILE)]

    def nn(a, b):
        return lax.dot_general(a, b, (((1,), (0,)), ((), ())), preferred_element_type=f32)

    def nt(a, b):
        return lax.dot_general(a, b, (((1,), (1,)), ((), ())), preferred_element_type=f32)

    def split(w, rows):
        return [(0, rows)] if w == TILE else [(0, rows // 2), (rows // 2, rows // 2)]

    def kernel(cnt_hbm, r_hbm, m_hbm, u_hbm, v_hbm, u_out, v_out,
               cnt, r_buf, m_buf, r_t, m_t, ut_f, ut_b, v_slot, v_send, v_f, e_b, vt_b,
               blk_sem, u_sem, v_sem, cnt_sem, recv_sem, send_sem):
        me = lax.axis_index("shard")
        left, right = lax.rem(me + n - 1, n), lax.rem(me + 1, n)

        barrier = pltpu.get_barrier_semaphore()
        for peer in (left, right):
            pl.semaphore_signal(barrier, inc=1, device_id={"shard": peer}, device_id_type=pl.DeviceIdType.MESH)

        def block_copy(kind, q):
            src, dst = ((r_hbm, r_buf), (m_hbm, m_buf))[kind]
            col = pl.multiple_of(lax.rem(me + q, n) * items, items)
            return pltpu.make_async_copy(src.at[:, pl.ds(col, items)], dst.at[q], blk_sem.at[kind, min(q, 1)])

        def block_wait(first, count):
            for kind, buf in enumerate((r_buf, m_buf)):
                blocks = buf.at[pl.ds(first, count)]
                pltpu.make_async_copy(blocks, blocks, blk_sem.at[kind, min(first, 1)]).wait()

        u_in = pltpu.make_async_copy(u_hbm, u_out, u_sem)
        v_in = pltpu.make_async_copy(v_hbm, v_slot.at[0], v_sem)
        cnt_in = pltpu.make_async_copy(cnt_hbm, cnt, cnt_sem)
        u_in.start()
        block_copy(0, 0).start()
        block_copy(1, 0).start()
        v_in.start()
        cnt_in.start()

        def flip_block(q):
            for s in range(0, users, 128):
                rows, cols = pl.ds(s, 128), pl.ds(s, 128)
                marked = jnp.where(m_buf[q, rows, :] != 0, r_buf[q, rows, :], jnp.nan).T
                r_t[q, :, cols] = marked
                m_t[q, :, cols] = jnp.where(marked == marked, 1.0, 0.0).astype(bf16)

        u_in.wait()
        for s in range(0, users, 128):
            flipped = u_out[pl.ds(s, 128), :].T
            ut_f[:, pl.ds(s, 128)] = flipped
            ut_b[:, pl.ds(s, 128)] = flipped.astype(bf16)
        block_wait(0, 1)
        for q in range(1, n):
            block_copy(0, q).start()
            block_copy(1, q).start()
        flip_block(0)
        v_in.wait()
        cnt_in.wait()

        def hop_copy(t, last=False):
            return pltpu.make_async_remote_copy(
                src_ref=v_send.at[lax.rem(t, 2)], dst_ref=v_out if last else v_slot.at[t + 1],
                send_sem=send_sem.at[lax.rem(t, 2)], recv_sem=recv_sem.at[lax.rem(t, n)],
                device_id={"shard": left}, device_id_type=pl.DeviceIdType.MESH)

        def when(condition, action):
            if isinstance(condition, bool):
                if condition:
                    action()
            else:
                pl.when(condition)(action)

        def sub_epoch(t, carry):
            q = lax.rem(t, n)
            count = cnt[0, lax.rem(me + t, n)]

            when(t > 0, lambda: hop_copy(t - 1).wait_recv())

            for k in range(STEPS_MAX):
                v_old = (v_slot.at[t] if k == 0 else v_f)[...]
                v_half = v_old.astype(bf16)
                if k == 0:
                    limit, keep_k = 0.5, keep
                    vt_b[...] = v_half.T
                else:
                    live = count > k
                    limit = jnp.where(live, 0.5, 2.0)
                    keep_k = jnp.where(live, keep, 1.0)
                    v_live = jnp.where(jnp.full(v_half.shape, count, jnp.int32) > k, v_old, 0.0).astype(bf16)
                    vt_b[...] = v_live.T

                def pick(new, old):
                    if k == 0:
                        return new
                    return jnp.where(jnp.full(new.shape, count, jnp.int32) > k, new, old)

                for s, w in tiles:
                    cols = pl.ds(s, w)
                    for a, h in split(w, items):
                        approx = nn(v_half[a:a + h], ut_b[:, cols])
                        err = (approx - r_t[q, pl.ds(a, h), cols]).astype(bf16)
                        seen = m_t[q, pl.ds(a, h), cols] > jnp.full((h, w), limit, f32).astype(bf16)
                        e_b[pl.ds(a, h), cols] = jnp.where(seen, err, jnp.zeros_like(err))
                half = items // 2
                parts = [keep * v_old[i * half:(i + 1) * half] for i in range(2)]

                def item_grad(s, w):
                    cols = pl.ds(s, w)
                    if w == TILE:
                        g = step_size * nt(e_b[:, cols], ut_b[:, cols])
                        for i in range(2):
                            parts[i] = parts[i] - g[i * half:(i + 1) * half]
                    else:
                        for i in range(2):
                            parts[i] = parts[i] - step_size * nt(e_b[pl.ds(i * half, half), cols], ut_b[:, cols])

                def item_update():
                    v_new = pick(jnp.concatenate(parts, axis=0), v_old)
                    if k < STEPS_MAX - 1:
                        v_f[...] = v_new
                    else:
                        if isinstance(t, int):
                            pl.semaphore_wait(barrier, 2)
                        v_send[lax.rem(t, 2)] = v_new
                        when(t < hops - 1, lambda: hop_copy(t).start())
                        when(t == hops - 1, lambda: hop_copy(t, last=True).start())

                def user_update(s, w):
                    cols = pl.ds(s, w)
                    for a, h in split(w, rank):
                        rows = pl.ds(a, h)
                        grad = nn(vt_b[rows, :], e_b[:, cols])
                        u_new = keep_k * ut_f[rows, cols] - step_size * grad
                        ut_f[rows, cols] = u_new
                        ut_b[rows, cols] = u_new.astype(bf16)

                wide = [x for x in tiles if x[1] == TILE]
                narrow = [x for x in tiles if x[1] < TILE]
                if k < STEPS_MAX - 1:
                    order = [(item_grad, wide), (user_update, wide), (item_grad, narrow), (item_update, None), (user_update, narrow)]
                else:
                    order = [(item_grad, wide), (item_grad, narrow), (item_update, None), (user_update, wide), (user_update, narrow)]
                for piece, group in order:
                    if group is None:
                        piece()
                    else:
                        for x in group:
                            piece(*x)

            if isinstance(t, int):
                block_wait(1, n - 1)
            when(t + 1 < n, lambda: flip_block(t + 1))
            when(t > 0, lambda: hop_copy(t - 1).wait_send())

            return carry

        sub_epoch(0, 0)
        lax.fori_loop(1, hops, sub_epoch, 0)
        for s in range(0, users, 128):
            u_out[pl.ds(s, 128), :] = ut_f[:, pl.ds(s, 128)].T
        hop_copy(hops - 1, last=True).wait_recv()
        hop_copy(hops - 1, last=True).wait_send()

    return kernel


def flush(u_vmem, v_vmem, u_out, v_out, sem):
    copies = [pltpu.make_async_copy(u_vmem, u_out, sem.at[0]), pltpu.make_async_copy(v_vmem, v_out, sem.at[1])]
    for copy in copies:
        copy.start()
    for copy in copies:
        copy.wait()


def solution(mesh):
    n = mesh.shape["shard"]
    row_spec = P(("rep", "shard"), None)
    hops = EPOCHS * n

    def local_run(ratings, obs_mask, step_counts, user_init, item_init):
        users, rank = user_init.shape
        items = item_init.shape[0]
        f32, bf16 = jnp.float32, jnp.bfloat16
        dma = pltpu.SemaphoreType.DMA
        hbm = pl.BlockSpec(memory_space=pl.ANY)
        vmem = pl.BlockSpec(memory_space=pltpu.VMEM)
        factors = pl.pallas_call(
            make_kernel(n, users, items, rank),
            out_shape=(pltpu.VMEM((users, rank), f32), pltpu.VMEM((items, rank), f32)),
            in_specs=[hbm, hbm, hbm, hbm, hbm],
            out_specs=(vmem, vmem),
            scratch_shapes=[
                pltpu.SMEM((1, n), jnp.int32),
                pltpu.VMEM((n, users, items), f32),
                pltpu.VMEM((n, users, items), jnp.int32),
                pltpu.VMEM((n, items, users), f32),
                pltpu.VMEM((n, items, users), bf16),
                pltpu.VMEM((rank, users), f32),
                pltpu.VMEM((rank, users), bf16),
                pltpu.VMEM((hops, items, rank), f32),
                pltpu.VMEM((2, items, rank), f32),
                pltpu.VMEM((items, rank), f32),
                pltpu.VMEM((items, users), bf16),
                pltpu.VMEM((rank, items), bf16),
                dma((2, 2)), dma, dma, dma, dma((n,)), dma((2,)),
            ],
            compiler_params=pltpu.CompilerParams(collective_id=0, has_side_effects=True),
            name="dsgd",
        )(step_counts, ratings, obs_mask, user_init, item_init)
        return pl.pallas_call(
            flush,
            out_shape=(jax.ShapeDtypeStruct((users, rank), f32), jax.ShapeDtypeStruct((items, rank), f32)),
            in_specs=[vmem, vmem],
            out_specs=(hbm, hbm),
            scratch_shapes=[dma((2,))],
            compiler_params=pltpu.CompilerParams(vmem_limit_bytes=1 << 20),
            name="flush",
        )(*(pltpu.with_memory_space_constraint(x, pltpu.VMEM) for x in factors))

    return jax.shard_map(local_run, mesh=mesh, in_specs=(row_spec,) * 5, out_specs=(row_spec, row_spec), check_vma=False)
```

```python
import math
import jax
import jax.numpy as jnp
from jax import lax
from jax.experimental import pallas as pl
from jax.experimental.pallas import tpu as pltpu
from jax.sharding import PartitionSpec as P

EPOCHS = 2
STEPS_MAX = 4
TILE = 256


def make_kernel(n, users, items, rank):
    step_size = 0.4 * math.sqrt(rank) / (users + rank)
    decay = 0.1 * items / math.sqrt(rank)
    keep = 1.0 - step_size * decay
    hops = EPOCHS * n
    bf16, f32 = jnp.bfloat16, jnp.float32
    tiles = [(s, min(TILE, users - s)) for s in range(0, users, TILE)]

    def nn(a, b):
        return lax.dot_general(a, b, (((1,), (0,)), ((), ())), preferred_element_type=f32)

    def nt(a, b):
        return lax.dot_general(a, b, (((1,), (1,)), ((), ())), preferred_element_type=f32)

    def split(w, rows):
        return [(0, rows)] if w == TILE else [(0, rows // 2), (rows // 2, rows // 2)]

    def kernel(cnt_hbm, r_hbm, m_hbm, u_hbm, v_hbm, u_out, v_out,
               cnt, r_buf, m_buf, r_t, m_t, ut_f, ut_b, v_slot, v_send, v_f, e_b, vt_b,
               blk_sem, u_sem, v_sem, cnt_sem, recv_sem, send_sem):
        me = lax.axis_index("shard")
        left, right = lax.rem(me + n - 1, n), lax.rem(me + 1, n)

        barrier = pltpu.get_barrier_semaphore()
        for peer in (left, right):
            pl.semaphore_signal(barrier, inc=1, device_id={"shard": peer}, device_id_type=pl.DeviceIdType.MESH)

        def block_copy(kind, q):
            src, dst = ((r_hbm, r_buf), (m_hbm, m_buf))[kind]
            col = pl.multiple_of(lax.rem(me + q, n) * items, items)
            return pltpu.make_async_copy(src.at[:, pl.ds(col, items)], dst.at[q], blk_sem.at[kind, min(q, 1)])

        def block_wait(first, count):
            for kind, buf in enumerate((r_buf, m_buf)):
                blocks = buf.at[pl.ds(first, count)]
                pltpu.make_async_copy(blocks, blocks, blk_sem.at[kind, min(first, 1)]).wait()

        u_in = pltpu.make_async_copy(u_hbm, u_out, u_sem)
        v_in = pltpu.make_async_copy(v_hbm, v_slot.at[0], v_sem)
        cnt_in = pltpu.make_async_copy(cnt_hbm, cnt, cnt_sem)
        u_in.start()
        block_copy(0, 0).start()
        block_copy(1, 0).start()
        v_in.start()
        cnt_in.start()

        def flip_block(q):
            for s in range(0, users, 128):
                rows, cols = pl.ds(s, 128), pl.ds(s, 128)
                marked = jnp.where(m_buf[q, rows, :] != 0, r_buf[q, rows, :], jnp.nan).T
                r_t[q, :, cols] = marked
                m_t[q, :, cols] = jnp.where(marked == marked, 1.0, 0.0).astype(bf16)

        def flip_users():
            for s in range(0, users, 128):
                flipped = u_out[pl.ds(s, 128), :].T
                ut_f[:, pl.ds(s, 128)] = flipped
                ut_b[:, pl.ds(s, 128)] = flipped.astype(bf16)

        u_in.wait()
        v_in.wait()
        cnt_in.wait()
        block_wait(0, 1)
        for q in range(1, n):
            block_copy(0, q).start()
            block_copy(1, q).start()
        flip_block(0)

        def hop_copy(t, last=False):
            return pltpu.make_async_remote_copy(
                src_ref=v_send.at[lax.rem(t, 2)], dst_ref=v_out if last else v_slot.at[t + 1],
                send_sem=send_sem.at[lax.rem(t, 2)], recv_sem=recv_sem.at[lax.rem(t, n)],
                device_id={"shard": left}, device_id_type=pl.DeviceIdType.MESH)

        def when(condition, action):
            if isinstance(condition, bool):
                if condition:
                    action()
            else:
                pl.when(condition)(action)

        def sub_epoch(t, carry):
            q = lax.rem(t, n)
            count = cnt[0, lax.rem(me + t, n)]

            when(t > 0, lambda: hop_copy(t - 1).wait_recv())

            for k in range(STEPS_MAX):
                v_old = (v_slot.at[t] if k == 0 else v_f)[...]
                v_half = v_old.astype(bf16)
                if k == 0:
                    limit, keep_k = 0.5, keep
                    vt_b[...] = v_half.T
                else:
                    live = count > k
                    limit = jnp.where(live, 0.5, 2.0)
                    keep_k = jnp.where(live, keep, 1.0)
                    v_live = jnp.where(jnp.full(v_half.shape, count, jnp.int32) > k, v_old, 0.0).astype(bf16)
                    vt_b[...] = v_live.T

                def pick(new, old):
                    if k == 0:
                        return new
                    return jnp.where(jnp.full(new.shape, count, jnp.int32) > k, new, old)

                fresh = isinstance(t, int) and k == 0
                for s, w in tiles:
                    cols = pl.ds(s, w)
                    for a, h in split(w, items):
                        if fresh:
                            approx = nt(v_half[a:a + h], u_out[cols, :].astype(bf16))
                        else:
                            approx = nn(v_half[a:a + h], ut_b[:, cols])
                        err = (approx - r_t[q, pl.ds(a, h), cols]).astype(bf16)
                        seen = m_t[q, pl.ds(a, h), cols] > jnp.full((h, w), limit, f32).astype(bf16)
                        e_b[pl.ds(a, h), cols] = jnp.where(seen, err, jnp.zeros_like(err))
                half = items // 2
                parts = [keep * v_old[i * half:(i + 1) * half] for i in range(2)]

                def times_users(err, cols):
                    return nn(err, u_out[cols, :].astype(bf16)) if fresh else nt(err, ut_b[:, cols])

                def item_grad(s, w):
                    cols = pl.ds(s, w)
                    if w == TILE:
                        g = step_size * times_users(e_b[:, cols], cols)
                        for i in range(2):
                            parts[i] = parts[i] - g[i * half:(i + 1) * half]
                    else:
                        for i in range(2):
                            parts[i] = parts[i] - step_size * times_users(e_b[pl.ds(i * half, half), cols], cols)

                def item_update():
                    v_new = pick(jnp.concatenate(parts, axis=0), v_old)
                    if k < STEPS_MAX - 1:
                        v_f[...] = v_new
                    else:
                        if isinstance(t, int):
                            pl.semaphore_wait(barrier, 2)
                        v_send[lax.rem(t, 2)] = v_new
                        when(t < hops - 1, lambda: hop_copy(t).start())
                        when(t == hops - 1, lambda: hop_copy(t, last=True).start())

                def user_update(s, w):
                    cols = pl.ds(s, w)
                    for a, h in split(w, rank):
                        rows = pl.ds(a, h)
                        grad = nn(vt_b[rows, :], e_b[:, cols])
                        u_new = keep_k * ut_f[rows, cols] - step_size * grad
                        ut_f[rows, cols] = u_new
                        ut_b[rows, cols] = u_new.astype(bf16)

                if fresh:
                    flip_users()
                wide = [x for x in tiles if x[1] == TILE]
                narrow = [x for x in tiles if x[1] < TILE]
                if k < STEPS_MAX - 1:
                    order = [(item_grad, wide), (user_update, wide), (item_grad, narrow), (item_update, None), (user_update, narrow)]
                else:
                    order = [(item_grad, wide), (item_grad, narrow), (item_update, None), (user_update, wide), (user_update, narrow)]
                for piece, group in order:
                    if group is None:
                        piece()
                    else:
                        for x in group:
                            piece(*x)

            if isinstance(t, int):
                block_wait(1, n - 1)
            when(t + 1 < n, lambda: flip_block(t + 1))
            when(t > 0, lambda: hop_copy(t - 1).wait_send())

            return carry

        sub_epoch(0, 0)
        lax.fori_loop(1, hops, sub_epoch, 0)
        for s in range(0, users, 128):
            u_out[pl.ds(s, 128), :] = ut_f[:, pl.ds(s, 128)].T
        hop_copy(hops - 1, last=True).wait_recv()
        hop_copy(hops - 1, last=True).wait_send()

    return kernel


def flush(u_vmem, v_vmem, u_out, v_out, sem):
    copies = [pltpu.make_async_copy(u_vmem, u_out, sem.at[0]), pltpu.make_async_copy(v_vmem, v_out, sem.at[1])]
    for copy in copies:
        copy.start()
    for copy in copies:
        copy.wait()


def solution(mesh):
    n = mesh.shape["shard"]
    row_spec = P(("rep", "shard"), None)
    hops = EPOCHS * n

    def local_run(ratings, obs_mask, step_counts, user_init, item_init):
        users, rank = user_init.shape
        items = item_init.shape[0]
        f32, bf16 = jnp.float32, jnp.bfloat16
        dma = pltpu.SemaphoreType.DMA
        hbm = pl.BlockSpec(memory_space=pl.ANY)
        vmem = pl.BlockSpec(memory_space=pltpu.VMEM)
        factors = pl.pallas_call(
            make_kernel(n, users, items, rank),
            out_shape=(pltpu.VMEM((users, rank), f32), pltpu.VMEM((items, rank), f32)),
            in_specs=[hbm, hbm, hbm, hbm, hbm],
            out_specs=(vmem, vmem),
            scratch_shapes=[
                pltpu.SMEM((1, n), jnp.int32),
                pltpu.VMEM((n, users, items), f32),
                pltpu.VMEM((n, users, items), jnp.int32),
                pltpu.VMEM((n, items, users), f32),
                pltpu.VMEM((n, items, users), bf16),
                pltpu.VMEM((rank, users), f32),
                pltpu.VMEM((rank, users), bf16),
                pltpu.VMEM((hops, items, rank), f32),
                pltpu.VMEM((2, items, rank), f32),
                pltpu.VMEM((items, rank), f32),
                pltpu.VMEM((items, users), bf16),
                pltpu.VMEM((rank, items), bf16),
                dma((2, 2)), dma, dma, dma, dma((n,)), dma((2,)),
            ],
            compiler_params=pltpu.CompilerParams(collective_id=0, has_side_effects=True),
            name="dsgd",
        )(step_counts, ratings, obs_mask, user_init, item_init)
        return pl.pallas_call(
            flush,
            out_shape=(jax.ShapeDtypeStruct((users, rank), f32), jax.ShapeDtypeStruct((items, rank), f32)),
            in_specs=[vmem, vmem],
            out_specs=(hbm, hbm),
            scratch_shapes=[dma((2,))],
            compiler_params=pltpu.CompilerParams(vmem_limit_bytes=1 << 20),
            name="flush",
        )(*(pltpu.with_memory_space_constraint(x, pltpu.VMEM) for x in factors))

    return jax.shard_map(local_run, mesh=mesh, in_specs=(row_spec,) * 5, out_specs=(row_spec, row_spec), check_vma=False)
```
